16 devices in a mesh: dp: 4 (over y, z, core), tp: 4 (over x).
Axes of the slice: x: 4, y: 2, z: 1, core: 2. Of those that a mesh axis runs over, the one named last changes fastest.
The devices are a block of a 4x4x8 slice.
Arguments:
- x: bfloat16 [4096, 7168], P(('dp', 'tp')), parts along dimension 0
- gain: bfloat16 [7168], replicated
- wq: bfloat16 [7168, 7168], P(None, 'tp')
- wk: bfloat16 [7168, 1024], P(None, 'tp')
- wv: bfloat16 [7168, 1024], P(None, 'tp')
- wo: bfloat16 [7168, 7168], P('tp')
Outputs:
- output: bfloat16 [4096, 7168], P(('dp', 'tp')), parts along dimension 0
There are 4 independent parts. The reference program is written for one: setup_inputs(seed, part) draws one part's arguments, and reference() takes and returns one part's arrays. A program takes and returns all parts, laid end to end along the dimension named above; an argument that names none is the same for every part.
All inputs are finite; a program needn't handle non-finite values.
Results may differ from the reference program's by a relative error of at most 0.012.
Values are sent between devices in bfloat16 or wider.
A program may use at most 768 MiB of HBM per device.

```python
import jax
import jax.numpy as jnp
from jax import lax

ROWS = 1024
D = 7168
HEADS = 56
KV_HEADS = 8
HEAD = 128
THETA = 10000


def setup_inputs(seed: int = 0, part: int = 0) -> dict:
    kx, kn, kq, kk, kv, ko = jax.random.split(jax.random.key(seed), 6)

    def weights(key, rows, columns):
        return jax.random.normal(key, (rows, columns), jnp.float32) * rows**-0.5

    drawn = {
        "x": jax.random.normal(jax.random.fold_in(kx, part), (ROWS, D), jnp.float32),
        "gain": 1 + 0.1 * jax.random.normal(kn, (D,), jnp.float32),
        "wq": 2 * weights(kq, D, HEADS * HEAD),
        "wk": 2 * weights(kk, D, KV_HEADS * HEAD),
        "wv": 4 * weights(kv, D, KV_HEADS * HEAD),
        "wo": weights(ko, HEADS * HEAD, D),
    }
    return {k: v.astype(jnp.bfloat16) for k, v in drawn.items()}


def normed(x, gain):
    wide = x.astype(jnp.float32)
    scale = lax.rsqrt(jnp.mean(wide * wide, -1, keepdims=True) + 1e-6)
    return (wide * scale * gain.astype(jnp.float32)).astype(jnp.bfloat16)


def turned(t, place, theta):
    half = t.shape[-1] // 2
    angle = place.astype(jnp.float32)[:, None] * theta ** (-jnp.arange(half, dtype=jnp.float32) / half)
    cos, sin = jnp.cos(angle)[:, None], jnp.sin(angle)[:, None]
    a, b = t[..., :half].astype(jnp.float32), t[..., half:].astype(jnp.float32)
    return jnp.concatenate([a * cos - b * sin, b * cos + a * sin], -1).astype(jnp.bfloat16)


def matmul(a, w):
    return jnp.dot(a, w, preferred_element_type=jnp.float32).astype(jnp.bfloat16)


def einsum(form, a, b):
    return jnp.einsum(form, a.astype(jnp.float32), b.astype(jnp.float32))


def attention(q, k, v):
    scores = einsum("tgsd,ugd->gstu", q, k) * q.shape[-1] ** -0.5
    token = jnp.arange(q.shape[0])
    scores = jnp.where(token[:, None] >= token, scores, -jnp.inf)
    weights = jax.nn.softmax(scores, -1).astype(jnp.bfloat16)
    return einsum("gstu,ugd->tgsd", weights, v).astype(jnp.bfloat16)


def reference(x, gain, wq, wk, wv, wo):
    a, place = normed(x, gain), jnp.arange(ROWS)
    q = turned(matmul(a, wq).reshape(ROWS, HEADS, HEAD), place, THETA).reshape(ROWS, KV_HEADS, -1, HEAD)
    k = turned(matmul(a, wk).reshape(ROWS, KV_HEADS, HEAD), place, THETA)
    v = matmul(a, wv).reshape(ROWS, KV_HEADS, HEAD)
    seen = attention(q, k, v).reshape(ROWS, HEADS * HEAD)
    return (x.astype(jnp.float32) + jnp.dot(seen, wo, preferred_element_type=jnp.float32)).astype(jnp.bfloat16)
```

```python
import functools

import jax
import jax.numpy as jnp
import numpy as np
from jax import lax
from jax.experimental import pallas as pl
from jax.experimental.pallas import tpu as pltpu
from jax.sharding import PartitionSpec as P

HEAD = 128
THETA = 10000
NEG = -1e30
HIDDEN = 2 * NEG
LOG2E = 1.4426950408889634
VMEM = 67_000_000
MESH = pl.DeviceIdType.MESH

TILE = 256
PIECES = 4
SLOTS = 3
KEYS = 256
FIRST, PASSED, SECOND = 0, 1, 2
OWN, VIA, SUM = 0, 1, 2


def _dot(a, b, ca=1, cb=0):
    return lax.dot_general(a, b, (((ca,), (cb,)), ((), ())), preferred_element_type=jnp.float32)


def _kernel(n, heads, kv, x_ref, gain_ref, turn_ref, wq_ref, wk_ref, wv_ref, wo_ref, y_ref,
            xs, nb, qkv, sends, recvs, own, wbuf, turn, gain, top_s, mix_s,
            ag_send, ag_recv, rs_send, rs_recv, wsem, lsem, ysem):
    me = lax.axis_index("tp")
    right, left, far = lax.rem(me + 1, n), lax.rem(me + n - 1, n), lax.rem(me + 2, n)
    sides = ((right, left), (left, right))
    rows, width = x_ref.shape
    half, sub = rows // 2, rows // 4
    group = heads // kv
    inner = heads * HEAD
    depth = width // PIECES
    q_tiles = inner // TILE
    span = PIECES * TILE
    spans = width // span

    load_x = pltpu.make_async_copy(x_ref, xs.at[pl.ds(pl.multiple_of(me * rows, rows), rows)], lsem.at[0])
    load_turn = pltpu.make_async_copy(turn_ref, turn, lsem.at[1])
    load_gain = pltpu.make_async_copy(gain_ref, gain, lsem.at[2])

    def fetch_q(j, slot):
        @pl.when(j < q_tiles)
        def _():
            at = pl.ds(pl.multiple_of(j * TILE, TILE), TILE)
            pltpu.make_async_copy(wq_ref.at[:, :, at], wbuf.at[slot], wsem.at[slot]).start()

        @pl.when(j == q_tiles)
        def _():
            pltpu.make_async_copy(wk_ref, wbuf.at[slot], wsem.at[slot]).start()

        @pl.when(j == q_tiles + 1)
        def _():
            pltpu.make_async_copy(wv_ref, wbuf.at[slot], wsem.at[slot]).start()

    def fetch_o(j, slot):
        for c in range(PIECES):
            at = pl.ds(pl.multiple_of(j * span + c * TILE, TILE), TILE)
            pltpu.make_async_copy(wo_ref.at[:, at], wbuf.at[slot, c], wsem.at[slot]).start()

    passes = (fetch_q, fetch_q, fetch_q, fetch_o, fetch_q, fetch_o, fetch_o, fetch_o)
    lengths = [q_tiles + 2 if f is fetch_q else spans for f in passes]

    def stream(index, body):
        fetch, length, before = passes[index], lengths[index], sum(lengths[:index])

        @pl.loop(0, length)
        def _(j):
            slot = lax.rem(before + j, SLOTS)
            pltpu.make_async_copy(wk_ref, wbuf.at[slot], wsem.at[slot]).wait()
            body(j, slot)

            @pl.when(j + SLOTS < length)
            def _():
                fetch(j + SLOTS, slot)

            if index + 1 < len(passes):
                @pl.when(j + SLOTS >= length)
                def _():
                    passes[index + 1](j + SLOTS - length, slot)

    def gathered(way, kind):
        source = sides[way][1]
        near = source * rows + way * half
        return pl.multiple_of(jnp.where(kind == PASSED, far * rows + way * half,
                                        jnp.where(kind == SECOND, source * rows + (1 - way) * half, near)), half)

    def arrival(way, kind, s):
        here = xs.at[pl.ds(pl.multiple_of(gathered(way, kind) + s * sub, sub), sub)]
        return pltpu.make_async_remote_copy(here, here, ag_send.at[way, kind, s], ag_recv.at[way, kind, s],
                                            device_id={"tp": sides[way][1]}, device_id_type=MESH)

    def gather(way, kind, s):
        if kind == PASSED:
            at = gathered(way, FIRST) + s * sub
            source = xs.at[pl.ds(pl.multiple_of(at, sub), sub)]
        else:
            place = (way if kind == FIRST else 1 - way) * half + s * sub
            at = me * rows + place
            source = x_ref.at[pl.ds(place, sub)]
        return pltpu.make_async_remote_copy(source, xs.at[pl.ds(pl.multiple_of(at, sub), sub)], ag_send.at[way, kind, s],
                                            ag_recv.at[way, kind, s], device_id={"tp": sides[way][0]}, device_id_type=MESH)

    def scatter(way, kind, buffer, turn_no, j):
        return pltpu.make_async_remote_copy(sends.at[way, buffer, j], recvs.at[way, kind, j], rs_send.at[way, turn_no, j],
                                            rs_recv.at[way, kind, j], device_id={"tp": sides[way][0]}, device_id_type=MESH)

    def project(index, places):
        for p, place in enumerate(places):
            @pl.loop(0, half // 16)
            def _(i):
                here = pl.ds(pl.multiple_of(place + i * 16, 16), 16)
                there = pl.ds(pl.multiple_of(p * half + i * 16, 16), 16)
                squares = jnp.zeros((16, span), jnp.float32)
                for c in range(spans):
                    wide = xs[here, c * span : (c + 1) * span].astype(jnp.float32)
                    squares += wide * wide
                scale = lax.rsqrt(jnp.sum(squares, -1, keepdims=True) * (1 / width) + 1e-6)
                for c in range(spans):
                    wide = xs[here, c * span : (c + 1) * span].astype(jnp.float32)
                    g = gain[:, c * span : (c + 1) * span].astype(jnp.float32)
                    nb[there, c * span : (c + 1) * span] = (wide * scale * g).astype(jnp.bfloat16)

        def body(j, slot):
            t = _dot(nb[:, :depth], wbuf[slot, 0])
            for c in range(1, PIECES):
                t += _dot(nb[:, c * depth : (c + 1) * depth], wbuf[slot, c])
            t = t.astype(jnp.bfloat16)
            for p, place in enumerate(places):
                here = pl.ds(place, half)
                for h in range(TILE // HEAD):
                    head = t[p * half : (p + 1) * half, h * HEAD : (h + 1) * HEAD]

                    @pl.when(j <= q_tiles)
                    def _():
                        wide = head.astype(jnp.float32)
                        turned = wide * turn[0, here, :] + pltpu.roll(wide, HEAD // 2, 1) * turn[1, here, :]
                        qkv[j * (TILE // HEAD) + h, here, :] = turned.astype(jnp.bfloat16)

                    @pl.when(j > q_tiles)
                    def _():
                        qkv[j * (TILE // HEAD) + h, here, :] = head

        stream(index, body)

    strips = [(g, list(range(g * group + i, min(g * group + i + 2, (g + 1) * group)))) for g in range(kv) for i in range(0, group, 2)]

    def attend(places):
        e = HEAD**-0.5 * LOG2E
        ones = jnp.ones((8, KEYS), jnp.bfloat16)

        @pl.loop(0, len(places))
        def _(unit):
            place = pl.multiple_of(jnp.where(unit == 0, places[0], places[1]), half)
            mine = pl.ds(place, half)
            top_s[...] = jnp.full(top_s.shape, NEG, jnp.float32)
            mix_s[...] = jnp.zeros(mix_s.shape, jnp.float32)

            def block(j, masked):
                here = pl.ds(pl.multiple_of(j * KEYS, KEYS), KEYS)
                scores, weights, keeps = [], [], []
                for g, hs in strips:
                    q = jnp.concatenate([qkv[h, mine, :] for h in hs], axis=0)
                    scores.append(_dot(qkv[heads + g, here, :], q, 1, 1))
                if masked:
                    shape = (KEYS, 2 * half)
                    gap = lax.rem(lax.broadcasted_iota(jnp.int32, shape, 1), half) - lax.broadcasted_iota(jnp.int32, shape, 0)
                    ok = gap >= j * KEYS - place
                for i, s in enumerate(scores):
                    wide = s.shape[1]
                    if masked:
                        s = jnp.where(ok[:, :wide], s, HIDDEN)
                    old = top_s[i : i + 1, :wide]
                    top = jnp.maximum(old, s.max(axis=0, keepdims=True))
                    top_s[i : i + 1, :wide] = top
                    weights.append(jnp.exp2((s - top) * e).astype(jnp.bfloat16))
                    keeps.append(jnp.exp2((old - top) * e))
                for i, (g, hs) in enumerate(strips):
                    wide = len(hs) * half
                    values = jnp.concatenate([qkv[heads + kv + g, here, :].T, ones], axis=0)
                    mix_s[i, :, :wide] = mix_s[i, :, :wide] * keeps[i] + _dot(values, weights[i])

            whole = lax.div(place, KEYS)

            @pl.loop(0, whole)
            def _(j):
                block(j, False)

            block(whole, True)
            for i, (g, hs) in enumerate(strips):
                wide = len(hs) * half
                out = (mix_s[i, :HEAD, :wide] * (1 / mix_s[i, HEAD : HEAD + 1, :wide])).T.astype(jnp.bfloat16)
                for m, h in enumerate(hs):
                    qkv[h, mine, :] = out[m * half : (m + 1) * half, :]

    def terms(index, places, before, emit):
        for p, place in enumerate(places):
            for h in range(heads):
                nb[p * half : (p + 1) * half, h * HEAD : (h + 1) * HEAD] = qkv[h, pl.ds(place, half), :]

        def body(j, slot):
            before(j)
            for c in range(PIECES):
                emit(j, slice(c * TILE, (c + 1) * TILE), _dot(nb[:, :inner], wbuf[slot, c]))

        stream(index, body)

    def send_terms(index, places, kinds, turn_no):
        buffer = turn_no % 2

        def before(j):
            @pl.when(j > 0)
            def _():
                for way in range(2):
                    scatter(way, kinds[way], buffer, turn_no, j - 1).start()

            if turn_no == 2:
                for way in range(2):
                    scatter(way, OWN, buffer, 0, j).wait_send()
                    scatter(way, VIA, buffer, turn_no, j).wait_recv()

        def emit(j, columns, t):
            for way in range(2):
                mine = t[way * half : (way + 1) * half]
                if turn_no == 2:
                    mine += recvs[way, VIA, j, :, columns].astype(jnp.float32)
                sends[way, buffer, j, :, columns] = mine.astype(jnp.bfloat16)

        terms(index, places, before, emit)
        for way in range(2):
            scatter(way, kinds[way], buffer, turn_no, spans - 1).start()

    load_x.start()
    load_gain.start()
    load_turn.start()
    for j in range(SLOTS):
        passes[0](jnp.int32(j), j)
    qkv[heads:] = jnp.zeros((2 * kv, *qkv.shape[1:]), jnp.bfloat16)

    barrier = pltpu.get_barrier_semaphore()
    for other in (left, right):
        pl.semaphore_signal(barrier, inc=1, device_id={"tp": other}, device_id_type=MESH)
    pl.semaphore_wait(barrier, 2)

    pass_first = (me > 0, me == n - 1)
    for s in range(2):
        for way in range(2):
            gather(way, FIRST, s).start()
    for s in range(2):
        for way in range(2):
            @pl.when(jnp.logical_not(pass_first[way]))
            def _():
                gather(way, SECOND, s).start()

    load_x.wait()
    load_gain.wait()
    load_turn.wait()
    project(0, (pl.multiple_of(me * rows, rows), pl.multiple_of(me * rows + half, half)))
    for s in range(2):
        for way in range(2):
            arrival(way, FIRST, s).wait_recv()
            gather(way, PASSED, s).start()
    for s in range(2):
        for way in range(2):
            @pl.when(pass_first[way])
            def _():
                gather(way, SECOND, s).start()
    project(1, (gathered(0, FIRST), gathered(1, FIRST)))

    second = (jnp.where(left > 0, PASSED, SECOND), jnp.where(right == n - 1, PASSED, SECOND))
    third = tuple(PASSED + SECOND - kind for kind in second)
    for index, kinds in ((2, second), (4, third)):
        for s in range(2):
            for way in range(2):
                arrival(way, kinds[way], s).wait_recv()
        project(index, (gathered(0, kinds[0]), gathered(1, kinds[1])))

        def scattered(way, kind):
            to = sides[way][0]
            return pl.multiple_of(jnp.where(kind == VIA, far * rows + (1 - way) * half,
                                            jnp.where(kind == OWN, to * rows + way * half, to * rows + (1 - way) * half)), half)

        early = tuple(jnp.where(sides[way][0] < far, OWN, VIA) for way in range(2))
        late = tuple(OWN + VIA - kind for kind in early)
        kinds = early if index == 2 else late
        places = tuple(scattered(way, kinds[way]) for way in range(2))
        attend(places)
        send_terms(index + 1, places, kinds, 0 if index == 2 else 1)

    kinds = (SUM, SUM)
    places = tuple(scattered(way, SUM) for way in range(2))
    attend(places)
    send_terms(6, places, kinds, 2)

    places = (pl.multiple_of(me * rows, rows), pl.multiple_of(me * rows + half, half))
    attend(places)

    def stage(j):
        return pl.ds(pl.multiple_of(inner + lax.rem(j, 2) * span, HEAD), span)

    def store_y(j):
        at = pl.ds(pl.multiple_of(j * span, span), span)
        return pltpu.make_async_copy(nb.at[:, stage(j)], y_ref.at[:, at], ysem.at[lax.rem(j, 2)])

    def finish(j, columns, t):
        own[:, columns] = t
        if columns.stop < span:
            return
        for way in range(2):
            for kind in (OWN, SUM):
                scatter(way, kind, 0, 2, j).wait_recv()

        @pl.when(j >= 2)
        def _():
            store_y(j - 2).wait()

        at = pl.ds(pl.multiple_of(j * span, span), span)
        for p in range(2):
            here = slice(p * half, (p + 1) * half)
            total = own[here, :] + xs[pl.ds(pl.multiple_of(places[p], half), half), at].astype(jnp.float32)
            total += recvs[p, OWN, j].astype(jnp.float32) + recvs[1 - p, SUM, j].astype(jnp.float32)
            nb[here, stage(j)] = total.astype(jnp.bfloat16)

        store_y(j).start()

    terms(7, places, lambda j: None, finish)

    for way in range(2):
        for kind in (FIRST, PASSED, SECOND):
            for s in range(2):
                gather(way, kind, s).wait_send()

    @pl.loop(0, spans)
    def _(j):
        for way in range(2):
            scatter(way, late[way], 1, 1, j).wait_send()
            scatter(way, SUM, 0, 2, j).wait_send()

    for j in range(spans - 2, spans):
        store_y(jnp.int32(j)).wait()


def _turns(tokens):
    half = HEAD // 2
    angle = np.arange(tokens, dtype=np.float32)[:, None] * np.float32(THETA) ** (-np.arange(half, dtype=np.float32) / np.float32(half))
    cos, sin = np.cos(angle.astype(np.float64)), np.sin(angle.astype(np.float64))
    return np.stack([np.concatenate([cos, cos], -1), np.concatenate([-sin, sin], -1)]).astype(np.float32)


def solution(mesh):
    n = mesh.shape["tp"]

    def step(x, gain, wq, wk, wv, wo):
        rows, width = x.shape
        inner, kv_inner = wq.shape[1], wk.shape[1]
        heads, kv = inner // HEAD, kv_inner // HEAD
        half, tokens, span = rows // 2, n * rows, PIECES * TILE
        spans, depth = width // span, width // PIECES
        strips = kv * -(-(heads // kv) // 2)
        bf16, f32 = jnp.bfloat16, jnp.float32
        anywhere = pl.BlockSpec(memory_space=pl.ANY)
        return pl.pallas_call(
            functools.partial(_kernel, n, heads, kv),
            out_shape=jax.ShapeDtypeStruct((rows, width), bf16),
            in_specs=[anywhere] * 7,
            out_specs=anywhere,
            scratch_shapes=[
                pltpu.VMEM((tokens, width), bf16),
                pltpu.VMEM((rows, width), bf16),
                pltpu.VMEM((heads + 2 * kv, tokens, HEAD), bf16),
                pltpu.VMEM((2, 2, spans, half, span), bf16),
                pltpu.VMEM((2, 3, spans, half, span), bf16),
                pltpu.VMEM((rows, span), f32),
                pltpu.VMEM((SLOTS, PIECES, depth, TILE), bf16),
                pltpu.VMEM((2, tokens, HEAD), f32),
                pltpu.VMEM((1, width), bf16),
                pltpu.VMEM((strips, 2 * half), f32),
                pltpu.VMEM((strips, HEAD + 8, 2 * half), f32),
                pltpu.SemaphoreType.DMA((2, 3, 2)),
                pltpu.SemaphoreType.DMA((2, 3, 2)),
                pltpu.SemaphoreType.DMA((2, 3, spans)),
                pltpu.SemaphoreType.DMA((2, 3, spans)),
                pltpu.SemaphoreType.DMA((SLOTS,)),
                pltpu.SemaphoreType.DMA((3,)),
                pltpu.SemaphoreType.DMA((2,)),
            ],
            compiler_params=pltpu.CompilerParams(collective_id=0, has_side_effects=True, vmem_limit_bytes=VMEM),
        )(x, gain[None], _turns(tokens), wq.reshape(PIECES, depth, inner), wk.reshape(PIECES, depth, kv_inner),
          wv.reshape(PIECES, depth, kv_inner), wo)

    tokens, columns = P(("dp", "tp"), None), P(None, "tp")
    return jax.shard_map(
        step,
        mesh=mesh,
        in_specs=(tokens, P(None), columns, columns, columns, P("tp", None)),
        out_specs=tokens,
        check_vma=False,
    )
```

```python
import functools

import jax
import jax.numpy as jnp
import numpy as np
from jax import lax
from jax.experimental import pallas as pl
from jax.experimental.pallas import tpu as pltpu
from jax.sharding import PartitionSpec as P

HEAD = 128
THETA = 10000
NEG = -1e30
HIDDEN = 2 * NEG
LOG2E = 1.4426950408889634
VMEM = 63_000_000
MESH = pl.DeviceIdType.MESH

TILE = 256
PIECES = 4
SLOTS = 3
KEYS = 256
FIRST, PASSED, SECOND = 0, 1, 2
OWN, VIA, SUM = 0, 1, 2


def _dot(a, b, ca=1, cb=0):
    return lax.dot_general(a, b, (((ca,), (cb,)), ((), ())), preferred_element_type=jnp.float32)


def _kernel(n, heads, kv, x_ref, gain_ref, turn_ref, wq_ref, wk_ref, wv_ref, wo_ref, y_ref,
            xs, nb, qkv, sends, recvs, own, wbuf, turn, gain_in, gain, top_s, mix_s,
            ag_send, ag_recv, rs_send, rs_recv, wsem, lsem):
    me = lax.axis_index("tp")
    right, left, far = lax.rem(me + 1, n), lax.rem(me + n - 1, n), lax.rem(me + 2, n)
    sides = ((right, left), (left, right))
    rows, width = x_ref.shape
    half, sub = rows // 2, rows // 4
    group = heads // kv
    inner = heads * HEAD
    depth = width // PIECES
    q_tiles = inner // TILE
    span = PIECES * TILE
    spans = width // span

    load_x = pltpu.make_async_copy(x_ref, xs.at[pl.ds(pl.multiple_of(me * rows, rows), rows)], lsem.at[0])
    load_turn = pltpu.make_async_copy(turn_ref, turn, lsem.at[1])
    load_gain = pltpu.make_async_copy(gain_ref, gain_in, lsem.at[2])

    def fetch_q(j, slot):
        @pl.when(j < q_tiles)
        def _():
            at = pl.ds(pl.multiple_of(j * TILE, TILE), TILE)
            pltpu.make_async_copy(wq_ref.at[:, :, at], wbuf.at[slot], wsem.at[slot]).start()

        @pl.when(j == q_tiles)
        def _():
            pltpu.make_async_copy(wk_ref, wbuf.at[slot], wsem.at[slot]).start()

        @pl.when(j == q_tiles + 1)
        def _():
            pltpu.make_async_copy(wv_ref, wbuf.at[slot], wsem.at[slot]).start()

    def fetch_o(j, slot):
        for c in range(PIECES):
            at = pl.ds(pl.multiple_of(j * span + c * TILE, TILE), TILE)
            pltpu.make_async_copy(wo_ref.at[:, at], wbuf.at[slot, c], wsem.at[slot]).start()

    passes = (fetch_q, fetch_q, fetch_q, fetch_o, fetch_q, fetch_o, fetch_o, fetch_o)
    lengths = [q_tiles + 2 if f is fetch_q else spans for f in passes]

    def stream(index, body):
        fetch, length, before = passes[index], lengths[index], sum(lengths[:index])

        @pl.loop(0, length)
        def _(j):
            slot = lax.rem(before + j, SLOTS)
            pltpu.make_async_copy(wk_ref, wbuf.at[slot], wsem.at[slot]).wait()
            body(j, slot)

            @pl.when(j + SLOTS < length)
            def _():
                fetch(j + SLOTS, slot)

            if index + 1 < len(passes):
                @pl.when(j + SLOTS >= length)
                def _():
                    passes[index + 1](j + SLOTS - length, slot)

    def gathered(way, kind):
        source = sides[way][1]
        near = source * rows + way * half
        return pl.multiple_of(jnp.where(kind == PASSED, far * rows + way * half,
                                        jnp.where(kind == SECOND, source * rows + (1 - way) * half, near)), half)

    def arrival(way, kind, s):
        here = xs.at[pl.ds(pl.multiple_of(gathered(way, kind) + s * sub, sub), sub)]
        return pltpu.make_async_remote_copy(here, here, ag_send.at[way, kind, s], ag_recv.at[way, kind, s],
                                            device_id={"tp": sides[way][1]}, device_id_type=MESH)

    def gather(way, kind, s):
        if kind == PASSED:
            at = gathered(way, FIRST) + s * sub
            source = xs.at[pl.ds(pl.multiple_of(at, sub), sub)]
        else:
            place = (way if kind == FIRST else 1 - way) * half + s * sub
            at = me * rows + place
            source = x_ref.at[pl.ds(place, sub)]
        return pltpu.make_async_remote_copy(source, xs.at[pl.ds(pl.multiple_of(at, sub), sub)], ag_send.at[way, kind, s],
                                            ag_recv.at[way, kind, s], device_id={"tp": sides[way][0]}, device_id_type=MESH)

    def scatter(way, kind, buffer, turn_no, j):
        return pltpu.make_async_remote_copy(sends.at[way, buffer, j], recvs.at[way, kind, j], rs_send.at[way, turn_no, j],
                                            rs_recv.at[way, kind, j], device_id={"tp": sides[way][0]}, device_id_type=MESH)

    def project(index, places):
        for p, place in enumerate(places):
            @pl.loop(0, half // 16)
            def _(i):
                here = pl.ds(pl.multiple_of(place + i * 16, 16), 16)
                there = pl.ds(pl.multiple_of(p * half + i * 16, 16), 16)
                squares = jnp.zeros((16, span), jnp.float32)
                for c in range(spans):
                    wide = xs[here, c * span : (c + 1) * span].astype(jnp.float32)
                    squares += wide * wide
                scale = lax.rsqrt(jnp.sum(squares, -1, keepdims=True) * (1 / width) + 1e-6)
                for c in range(spans):
                    wide = xs[here, c * span : (c + 1) * span].astype(jnp.float32)
                    nb[there, c * span : (c + 1) * span] = (wide * scale * gain[:, c * span : (c + 1) * span]).astype(jnp.bfloat16)

        def body(j, slot):
            t = _dot(nb[:, :depth], wbuf[slot, 0])
            for c in range(1, PIECES):
                t += _dot(nb[:, c * depth : (c + 1) * depth], wbuf[slot, c])
            t = t.astype(jnp.bfloat16)
            for p, place in enumerate(places):
                here = pl.ds(place, half)
                for h in range(TILE // HEAD):
                    head = t[p * half : (p + 1) * half, h * HEAD : (h + 1) * HEAD]

                    @pl.when(j <= q_tiles)
                    def _():
                        wide = head.astype(jnp.float32)
                        turned = wide * turn[0, here, :] + pltpu.roll(wide, HEAD // 2, 1) * turn[1, here, :]
                        qkv[j * (TILE // HEAD) + h, here, :] = turned.astype(jnp.bfloat16)

                    @pl.when(j > q_tiles)
                    def _():
                        qkv[j * (TILE // HEAD) + h, here, :] = head

        stream(index, body)

    strips = [(g, list(range(g * group + i, min(g * group + i + 2, (g + 1) * group)))) for g in range(kv) for i in range(0, group, 2)]

    def attend(places):
        e = HEAD**-0.5 * LOG2E
        ones = jnp.ones((8, KEYS), jnp.bfloat16)

        @pl.loop(0, len(places))
        def _(unit):
            place = pl.multiple_of(jnp.where(unit == 0, places[0], places[1]), half)
            mine = pl.ds(place, half)
            top_s[...] = jnp.full(top_s.shape, NEG, jnp.float32)
            mix_s[...] = jnp.zeros(mix_s.shape, jnp.float32)

            def block(j, masked):
                here = pl.ds(pl.multiple_of(j * KEYS, KEYS), KEYS)
                scores, weights, keeps = [], [], []
                for g, hs in strips:
                    q = jnp.concatenate([qkv[h, mine, :] for h in hs], axis=0)
                    scores.append(_dot(qkv[heads + g, here, :], q, 1, 1))
                if masked:
                    shape = (KEYS, 2 * half)
                    gap = lax.rem(lax.broadcasted_iota(jnp.int32, shape, 1), half) - lax.broadcasted_iota(jnp.int32, shape, 0)
                    ok = gap >= j * KEYS - place
                for i, s in enumerate(scores):
                    wide = s.shape[1]
                    if masked:
                        s = jnp.where(ok[:, :wide], s, HIDDEN)
                    old = top_s[i : i + 1, :wide]
                    top = jnp.maximum(old, s.max(axis=0, keepdims=True))
                    top_s[i : i + 1, :wide] = top
                    weights.append(jnp.exp2((s - top) * e).astype(jnp.bfloat16))
                    keeps.append(jnp.exp2((old - top) * e))
                for i, (g, hs) in enumerate(strips):
                    wide = len(hs) * half
                    values = jnp.concatenate([qkv[heads + kv + g, here, :].T, ones], axis=0)
                    mix_s[i, :, :wide] = mix_s[i, :, :wide] * keeps[i] + _dot(values, weights[i])

            whole = lax.div(place, KEYS)

            @pl.loop(0, whole)
            def _(j):
                block(j, False)

            block(whole, True)
            for i, (g, hs) in enumerate(strips):
                wide = len(hs) * half
                out = (mix_s[i, :HEAD, :wide] * (1 / mix_s[i, HEAD : HEAD + 1, :wide])).T.astype(jnp.bfloat16)
                for m, h in enumerate(hs):
                    qkv[h, mine, :] = out[m * half : (m + 1) * half, :]

    def terms(index, places, before, emit):
        for p, place in enumerate(places):
            for h in range(heads):
                nb[p * half : (p + 1) * half, h * HEAD : (h + 1) * HEAD] = qkv[h, pl.ds(place, half), :]

        def body(j, slot):
            before(j)
            for c in range(PIECES):
                emit(j, slice(c * TILE, (c + 1) * TILE), _dot(nb[:, :inner], wbuf[slot, c]))

        stream(index, body)

    def send_terms(index, places, kinds, turn_no):
        buffer = turn_no % 2

        def before(j):
            @pl.when(j > 0)
            def _():
                for way in range(2):
                    scatter(way, kinds[way], buffer, turn_no, j - 1).start()

            if turn_no == 2:
                for way in range(2):
                    scatter(way, OWN, buffer, 0, j).wait_send()
                    scatter(way, VIA, buffer, turn_no, j).wait_recv()

        def emit(j, columns, t):
            for way in range(2):
                mine = t[way * half : (way + 1) * half]
                if turn_no == 2:
                    mine += recvs[way, VIA, j, :, columns].astype(jnp.float32)
                sends[way, buffer, j, :, columns] = mine.astype(jnp.bfloat16)

        terms(index, places, before, emit)
        for way in range(2):
            scatter(way, kinds[way], buffer, turn_no, spans - 1).start()

    barrier = pltpu.get_barrier_semaphore()
    for other in (left, right):
        pl.semaphore_signal(barrier, inc=1, device_id={"tp": other}, device_id_type=MESH)
    load_x.start()
    load_gain.start()
    load_turn.start()
    for j in range(SLOTS):
        passes[0](jnp.int32(j), j)
    pl.semaphore_wait(barrier, 2)

    pass_first = (me > 0, me == n - 1)
    for s in range(2):
        for way in range(2):
            gather(way, FIRST, s).start()
    for s in range(2):
        for way in range(2):
            @pl.when(jnp.logical_not(pass_first[way]))
            def _():
                gather(way, SECOND, s).start()

    qkv[heads:] = jnp.zeros((2 * kv, *qkv.shape[1:]), jnp.bfloat16)
    load_x.wait()
    load_gain.wait()
    load_turn.wait()
    wide_gain = gain_in[...].astype(jnp.float32)
    for i in range(width // HEAD):
        gain[:, i * HEAD : (i + 1) * HEAD] = wide_gain[i : i + 1, :]
    project(0, (pl.multiple_of(me * rows, rows), pl.multiple_of(me * rows + half, half)))
    for s in range(2):
        for way in range(2):
            arrival(way, FIRST, s).wait_recv()
            gather(way, PASSED, s).start()
    for s in range(2):
        for way in range(2):
            @pl.when(pass_first[way])
            def _():
                gather(way, SECOND, s).start()
    project(1, (gathered(0, FIRST), gathered(1, FIRST)))

    second = (jnp.where(left > 0, PASSED, SECOND), jnp.where(right == n - 1, PASSED, SECOND))
    third = tuple(PASSED + SECOND - kind for kind in second)
    for index, kinds in ((2, second), (4, third)):
        for s in range(2):
            for way in range(2):
                arrival(way, kinds[way], s).wait_recv()
        project(index, (gathered(0, kinds[0]), gathered(1, kinds[1])))

        def scattered(way, kind):
            to = sides[way][0]
            return pl.multiple_of(jnp.where(kind == VIA, far * rows + (1 - way) * half,
                                            jnp.where(kind == OWN, to * rows + way * half, to * rows + (1 - way) * half)), half)

        early = tuple(jnp.where(sides[way][0] < far, OWN, VIA) for way in range(2))
        late = tuple(OWN + VIA - kind for kind in early)
        kinds = early if index == 2 else late
        places = tuple(scattered(way, kinds[way]) for way in range(2))
        attend(places)
        send_terms(index + 1, places, kinds, 0 if index == 2 else 1)

    kinds = (SUM, SUM)
    places = tuple(scattered(way, SUM) for way in range(2))
    attend(places)
    send_terms(6, places, kinds, 2)

    places = (pl.multiple_of(me * rows, rows), pl.multiple_of(me * rows + half, half))
    attend(places)

    def finish(j, columns, t):
        own[:, columns] = t
        if columns.stop < span:
            return
        for way in range(2):
            for kind in (OWN, SUM):
                scatter(way, kind, 0, 2, j).wait_recv()

        at = pl.ds(pl.multiple_of(j * span, span), span)
        for p in range(2):
            here = slice(p * half, (p + 1) * half)
            total = own[here, :] + xs[pl.ds(pl.multiple_of(places[p], half), half), at].astype(jnp.float32)
            total += recvs[p, OWN, j].astype(jnp.float32) + recvs[1 - p, SUM, j].astype(jnp.float32)
            y_ref[here, at] = total.astype(jnp.bfloat16)

    terms(7, places, lambda j: None, finish)

    for way in range(2):
        for kind in (FIRST, PASSED, SECOND):
            for s in range(2):
                gather(way, kind, s).wait_send()

    @pl.loop(0, spans)
    def _(j):
        for way in range(2):
            scatter(way, late[way], 1, 1, j).wait_send()
            scatter(way, SUM, 0, 2, j).wait_send()


def _turns(tokens):
    half = HEAD // 2
    angle = np.arange(tokens, dtype=np.float32)[:, None] * np.float32(THETA) ** (-np.arange(half, dtype=np.float32) / np.float32(half))
    cos, sin = np.cos(angle.astype(np.float64)), np.sin(angle.astype(np.float64))
    return np.stack([np.concatenate([cos, cos], -1), np.concatenate([-sin, sin], -1)]).astype(np.float32)


def solution(mesh):
    n = mesh.shape["tp"]

    def step(x, gain, wq, wk, wv, wo):
        rows, width = x.shape
        inner, kv_inner = wq.shape[1], wk.shape[1]
        heads, kv = inner // HEAD, kv_inner // HEAD
        half, tokens, span = rows // 2, n * rows, PIECES * TILE
        spans, depth = width // span, width // PIECES
        strips = kv * -(-(heads // kv) // 2)
        bf16, f32 = jnp.bfloat16, jnp.float32
        anywhere = pl.BlockSpec(memory_space=pl.ANY)
        return pl.pallas_call(
            functools.partial(_kernel, n, heads, kv),
            out_shape=pltpu.VMEM((rows, width), bf16),
            in_specs=[anywhere] * 7,
            out_specs=pl.BlockSpec(memory_space=pltpu.VMEM),
            scratch_shapes=[
                pltpu.VMEM((tokens, width), bf16),
                pltpu.VMEM((rows, width), bf16),
                pltpu.VMEM((heads + 2 * kv, tokens, HEAD), bf16),
                pltpu.VMEM((2, 2, spans, half, span), bf16),
                pltpu.VMEM((2, 3, spans, half, span), bf16),
                pltpu.VMEM((rows, span), f32),
                pltpu.VMEM((SLOTS, PIECES, depth, TILE), bf16),
                pltpu.VMEM((2, tokens, HEAD), f32),
                pltpu.VMEM((width // HEAD, HEAD), bf16),
                pltpu.VMEM((1, width), f32),
                pltpu.VMEM((strips, 2 * half), f32),
                pltpu.VMEM((strips, HEAD + 8, 2 * half), f32),
                pltpu.SemaphoreType.DMA((2, 3, 2)),
                pltpu.SemaphoreType.DMA((2, 3, 2)),
                pltpu.SemaphoreType.DMA((2, 3, spans)),
                pltpu.SemaphoreType.DMA((2, 3, spans)),
                pltpu.SemaphoreType.DMA((SLOTS,)),
                pltpu.SemaphoreType.DMA((3,)),
            ],
            compiler_params=pltpu.CompilerParams(collective_id=0, has_side_effects=True, vmem_limit_bytes=VMEM),
        )(x, gain.reshape(width // HEAD, HEAD), _turns(tokens), wq.reshape(PIECES, depth, inner), wk.reshape(PIECES, depth, kv_inner),
          wv.reshape(PIECES, depth, kv_inner), wo)

    tokens, columns = P(("dp", "tp"), None), P(None, "tp")
    return jax.shard_map(
        step,
        mesh=mesh,
        in_specs=(tokens, P(None), columns, columns, columns, P("tp", None)),
        out_specs=tokens,
        check_vma=False,
    )
```

```python
import functools

import jax
import jax.numpy as jnp
import numpy as np
from jax import lax
from jax.experimental import pallas as pl
from jax.experimental.pallas import tpu as pltpu
from jax.sharding import PartitionSpec as P

HEAD = 128
THETA = 10000
NEG = -1e30
HIDDEN = 2 * NEG
LOG2E = 1.4426950408889634
VMEM = 63_000_000
MESH = pl.DeviceIdType.MESH

TILE = 256
PIECES = 4
SLOTS = 3
KEYS = 256
FIRST, PASSED, SECOND = 0, 1, 2
OWN, VIA, SUM = 0, 1, 2


def _dot(a, b, ca=1, cb=0):
    return lax.dot_general(a, b, (((ca,), (cb,)), ((), ())), preferred_element_type=jnp.float32)


def _kernel(n, heads, kv, x_ref, gain_ref, turn_ref, wq_ref, wk_ref, wv_ref, wo_ref, y_ref,
            xs, nb, qkv, sends, recvs, own, wbuf, turn, gain_in, gain, top_s, mix_s,
            ag_send, ag_recv, rs_send, rs_recv, wsem, xsem, lsem):
    me = lax.axis_index("tp")
    right, left, far = lax.rem(me + 1, n), lax.rem(me + n - 1, n), lax.rem(me + 2, n)
    sides = ((right, left), (left, right))
    rows, width = x_ref.shape
    half, sub = rows // 2, rows // 4
    group = heads // kv
    inner = heads * HEAD
    depth = width // PIECES
    q_tiles = inner // TILE
    span = PIECES * TILE
    spans = width // span

    load_turn = pltpu.make_async_copy(turn_ref, turn, lsem.at[0])
    load_gain = pltpu.make_async_copy(gain_ref, gain_in, lsem.at[1])

    def load_x(quarter):
        here = xs.at[pl.ds(pl.multiple_of(me * rows + quarter * sub, sub), sub)]
        return pltpu.make_async_copy(x_ref.at[pl.ds(quarter * sub, sub)], here, xsem.at[quarter])


    def fetch_q(j, slot):
        @pl.when(j < q_tiles)
        def _():
            at = pl.ds(pl.multiple_of(j * TILE, TILE), TILE)
            pltpu.make_async_copy(wq_ref.at[:, :, at], wbuf.at[slot], wsem.at[slot]).start()

        @pl.when(j == q_tiles)
        def _():
            pltpu.make_async_copy(wk_ref, wbuf.at[slot], wsem.at[slot]).start()

        @pl.when(j == q_tiles + 1)
        def _():
            pltpu.make_async_copy(wv_ref, wbuf.at[slot], wsem.at[slot]).start()

    def fetch_o(j, slot):
        for c in range(PIECES):
            at = pl.ds(pl.multiple_of(j * span + c * TILE, TILE), TILE)
            pltpu.make_async_copy(wo_ref.at[:, at], wbuf.at[slot, c], wsem.at[slot]).start()

    passes = (fetch_q, fetch_q, fetch_q, fetch_o, fetch_q, fetch_o, fetch_o, fetch_o)
    lengths = [q_tiles + 2 if f is fetch_q else spans for f in passes]

    def stream(index, body):
        fetch, length, before = passes[index], lengths[index], sum(lengths[:index])

        @pl.loop(0, length)
        def _(j):
            slot = lax.rem(before + j, SLOTS)
            pltpu.make_async_copy(wk_ref, wbuf.at[slot], wsem.at[slot]).wait()
            body(j, slot)

            @pl.when(j + SLOTS < length)
            def _():
                fetch(j + SLOTS, slot)

            if index + 1 < len(passes):
                @pl.when(j + SLOTS >= length)
                def _():
                    passes[index + 1](j + SLOTS - length, slot)

    def gathered(way, kind):
        source = sides[way][1]
        near = source * rows + way * half
        return pl.multiple_of(jnp.where(kind == PASSED, far * rows + way * half,
                                        jnp.where(kind == SECOND, source * rows + (1 - way) * half, near)), half)

    def arrival(way, kind, s):
        here = xs.at[pl.ds(pl.multiple_of(gathered(way, kind) + s * sub, sub), sub)]
        return pltpu.make_async_remote_copy(here, here, ag_send.at[way, kind, s], ag_recv.at[way, kind, s],
                                            device_id={"tp": sides[way][1]}, device_id_type=MESH)

    def gather(way, kind, s):
        if kind == PASSED:
            at = gathered(way, FIRST) + s * sub
        else:
            at = me * rows + (way if kind == FIRST else 1 - way) * half + s * sub
        here = xs.at[pl.ds(pl.multiple_of(at, sub), sub)]
        return pltpu.make_async_remote_copy(here, here, ag_send.at[way, kind, s], ag_recv.at[way, kind, s],
                                            device_id={"tp": sides[way][0]}, device_id_type=MESH)

    def scatter(way, kind, buffer, turn_no, j):
        return pltpu.make_async_remote_copy(sends.at[way, buffer, j], recvs.at[way, kind, j], rs_send.at[way, turn_no, j],
                                            rs_recv.at[way, kind, j], device_id={"tp": sides[way][0]}, device_id_type=MESH)

    def project(index, places):
        for p, place in enumerate(places):
            @pl.loop(0, half // 16)
            def _(i):
                here = pl.ds(pl.multiple_of(place + i * 16, 16), 16)
                there = pl.ds(pl.multiple_of(p * half + i * 16, 16), 16)
                squares = jnp.zeros((16, span), jnp.float32)
                for c in range(spans):
                    wide = xs[here, c * span : (c + 1) * span].astype(jnp.float32)
                    squares += wide * wide
                scale = lax.rsqrt(jnp.sum(squares, -1, keepdims=True) * (1 / width) + 1e-6)
                for c in range(spans):
                    wide = xs[here, c * span : (c + 1) * span].astype(jnp.float32)
                    nb[there, c * span : (c + 1) * span] = (wide * scale * gain[:, c * span : (c + 1) * span]).astype(jnp.bfloat16)

        def body(j, slot):
            t = _dot(nb[:, :depth], wbuf[slot, 0])
            for c in range(1, PIECES):
                t += _dot(nb[:, c * depth : (c + 1) * depth], wbuf[slot, c])
            t = t.astype(jnp.bfloat16)
            for p, place in enumerate(places):
                here = pl.ds(place, half)
                for h in range(TILE // HEAD):
                    head = t[p * half : (p + 1) * half, h * HEAD : (h + 1) * HEAD]

                    @pl.when(j <= q_tiles)
                    def _():
                        wide = head.astype(jnp.float32)
                        turned = wide * turn[0, here, :] + pltpu.roll(wide, HEAD // 2, 1) * turn[1, here, :]
                        qkv[j * (TILE // HEAD) + h, here, :] = turned.astype(jnp.bfloat16)

                    @pl.when(j > q_tiles)
                    def _():
                        qkv[j * (TILE // HEAD) + h, here, :] = head

        stream(index, body)

    strips = [(g, list(range(g * group + i, min(g * group + i + 2, (g + 1) * group)))) for g in range(kv) for i in range(0, group, 2)]

    def attend(places):
        e = HEAD**-0.5 * LOG2E
        ones = jnp.ones((8, KEYS), jnp.bfloat16)

        @pl.loop(0, len(places))
        def _(unit):
            place = pl.multiple_of(jnp.where(unit == 0, places[0], places[1]), half)
            mine = pl.ds(place, half)
            top_s[...] = jnp.full(top_s.shape, NEG, jnp.float32)
            mix_s[...] = jnp.zeros(mix_s.shape, jnp.float32)

            def block(j, masked):
                here = pl.ds(pl.multiple_of(j * KEYS, KEYS), KEYS)
                scores, weights, keeps = [], [], []
                for g, hs in strips:
                    q = jnp.concatenate([qkv[h, mine, :] for h in hs], axis=0)
                    scores.append(_dot(qkv[heads + g, here, :], q, 1, 1))
                if masked:
                    shape = (KEYS, 2 * half)
                    gap = lax.rem(lax.broadcasted_iota(jnp.int32, shape, 1), half) - lax.broadcasted_iota(jnp.int32, shape, 0)
                    ok = gap >= j * KEYS - place
                for i, s in enumerate(scores):
                    wide = s.shape[1]
                    if masked:
                        s = jnp.where(ok[:, :wide], s, HIDDEN)
                    old = top_s[i : i + 1, :wide]
                    top = jnp.maximum(old, s.max(axis=0, keepdims=True))
                    top_s[i : i + 1, :wide] = top
                    weights.append(jnp.exp2((s - top) * e).astype(jnp.bfloat16))
                    keeps.append(jnp.exp2((old - top) * e))
                for i, (g, hs) in enumerate(strips):
                    wide = len(hs) * half
                    values = jnp.concatenate([qkv[heads + kv + g, here, :].T, ones], axis=0)
                    mix_s[i, :, :wide] = mix_s[i, :, :wide] * keeps[i] + _dot(values, weights[i])

            whole = lax.div(place, KEYS)

            @pl.loop(0, whole)
            def _(j):
                block(j, False)

            block(whole, True)
            for i, (g, hs) in enumerate(strips):
                wide = len(hs) * half
                out = (mix_s[i, :HEAD, :wide] * (1 / mix_s[i, HEAD : HEAD + 1, :wide])).T.astype(jnp.bfloat16)
                for m, h in enumerate(hs):
                    qkv[h, mine, :] = out[m * half : (m + 1) * half, :]

    def terms(index, places, before, emit):
        for p, place in enumerate(places):
            for h in range(heads):
                nb[p * half : (p + 1) * half, h * HEAD : (h + 1) * HEAD] = qkv[h, pl.ds(place, half), :]

        def body(j, slot):
            before(j)
            for c in range(PIECES):
                emit(j, slice(c * TILE, (c + 1) * TILE), _dot(nb[:, :inner], wbuf[slot, c]))

        stream(index, body)

    def send_terms(index, places, kinds, turn_no):
        buffer = turn_no % 2

        def before(j):
            @pl.when(j > 0)
            def _():
                for way in range(2):
                    scatter(way, kinds[way], buffer, turn_no, j - 1).start()

            if turn_no == 2:
                for way in range(2):
                    scatter(way, OWN, buffer, 0, j).wait_send()
                    scatter(way, VIA, buffer, turn_no, j).wait_recv()

        def emit(j, columns, t):
            for way in range(2):
                mine = t[way * half : (way + 1) * half]
                if turn_no == 2:
                    mine += recvs[way, VIA, j, :, columns].astype(jnp.float32)
                sends[way, buffer, j, :, columns] = mine.astype(jnp.bfloat16)

        terms(index, places, before, emit)
        for way in range(2):
            scatter(way, kinds[way], buffer, turn_no, spans - 1).start()

    barrier = pltpu.get_barrier_semaphore()
    for other in (left, right):
        pl.semaphore_signal(barrier, inc=1, device_id={"tp": other}, device_id_type=MESH)
    for quarter in (0, 2, 1, 3):
        load_x(quarter).start()
    pl.semaphore_wait(barrier, 2)

    pass_first = (me > 0, me == n - 1)
    for s in range(2):
        for way in range(2):
            load_x(2 * way + s).wait()
            gather(way, FIRST, s).start()
    load_gain.start()
    for j in range(SLOTS):
        passes[0](jnp.int32(j), j)
    load_turn.start()
    for s in range(2):
        for way in range(2):
            @pl.when(jnp.logical_not(pass_first[way]))
            def _():
                gather(way, SECOND, s).start()

    qkv[heads:] = jnp.zeros((2 * kv, *qkv.shape[1:]), jnp.bfloat16)
    load_gain.wait()
    load_turn.wait()
    wide_gain = gain_in[...].astype(jnp.float32)
    for i in range(width // HEAD):
        gain[:, i * HEAD : (i + 1) * HEAD] = wide_gain[i : i + 1, :]
    project(0, (pl.multiple_of(me * rows, rows), pl.multiple_of(me * rows + half, half)))
    for s in range(2):
        for way in range(2):
            arrival(way, FIRST, s).wait_recv()
            gather(way, PASSED, s).start()
    for s in range(2):
        for way in range(2):
            @pl.when(pass_first[way])
            def _():
                gather(way, SECOND, s).start()
    project(1, (gathered(0, FIRST), gathered(1, FIRST)))

    second = (jnp.where(left > 0, PASSED, SECOND), jnp.where(right == n - 1, PASSED, SECOND))
    third = tuple(PASSED + SECOND - kind for kind in second)
    for index, kinds in ((2, second), (4, third)):
        for s in range(2):
            for way in range(2):
                arrival(way, kinds[way], s).wait_recv()
        project(index, (gathered(0, kinds[0]), gathered(1, kinds[1])))

        def scattered(way, kind):
            to = sides[way][0]
            return pl.multiple_of(jnp.where(kind == VIA, far * rows + (1 - way) * half,
                                            jnp.where(kind == OWN, to * rows + way * half, to * rows + (1 - way) * half)), half)

        early = tuple(jnp.where(sides[way][0] < far, OWN, VIA) for way in range(2))
        late = tuple(OWN + VIA - kind for kind in early)
        kinds = early if index == 2 else late
        places = tuple(scattered(way, kinds[way]) for way in range(2))
        attend(places)
        send_terms(index + 1, places, kinds, 0 if index == 2 else 1)

    kinds = (SUM, SUM)
    places = tuple(scattered(way, SUM) for way in range(2))
    attend(places)
    send_terms(6, places, kinds, 2)

    places = (pl.multiple_of(me * rows, rows), pl.multiple_of(me * rows + half, half))
    attend(places)

    def finish(j, columns, t):
        own[:, columns] = t
        if columns.stop < span:
            return
        at = pl.ds(pl.multiple_of(j * span, span), span)
        halves = (slice(0, half), slice(half, rows))
        for p in range(2):
            scatter(p, OWN, 0, 2, j).wait_recv()
            x_part = xs[pl.ds(pl.multiple_of(places[p], half), half), at].astype(jnp.float32)
            own[halves[p], :] = own[halves[p], :] + x_part + recvs[p, OWN, j].astype(jnp.float32)

        @pl.when(j > 0)
        def _():
            for way in range(2):
                scatter(way, SUM, 0, 2, j - 1).wait_send()

        for p in (1, 0):
            scatter(1 - p, SUM, 0, 2, j).wait_recv()
            y_ref[halves[p], at] = (own[halves[p], :] + recvs[1 - p, SUM, j].astype(jnp.float32)).astype(jnp.bfloat16)

    for way in range(2):
        for kind in (FIRST, PASSED, SECOND):
            for s in range(2):
                gather(way, kind, s).wait_send()

    @pl.loop(0, spans)
    def _(j):
        for way in range(2):
            scatter(way, late[way], 1, 1, j).wait_send()

    terms(7, places, lambda j: None, finish)
    for way in range(2):
        scatter(way, SUM, 0, 2, spans - 1).wait_send()


def _turns(tokens):
    half = HEAD // 2
    angle = np.arange(tokens, dtype=np.float32)[:, None] * np.float32(THETA) ** (-np.arange(half, dtype=np.float32) / np.float32(half))
    cos, sin = np.cos(angle.astype(np.float64)), np.sin(angle.astype(np.float64))
    return np.stack([np.concatenate([cos, cos], -1), np.concatenate([-sin, sin], -1)]).astype(np.float32)


def solution(mesh):
    n = mesh.shape["tp"]

    def step(x, gain, wq, wk, wv, wo):
        rows, width = x.shape
        inner, kv_inner = wq.shape[1], wk.shape[1]
        heads, kv = inner // HEAD, kv_inner // HEAD
        half, tokens, span = rows // 2, n * rows, PIECES * TILE
        spans, depth = width // span, width // PIECES
        strips = kv * -(-(heads // kv) // 2)
        bf16, f32 = jnp.bfloat16, jnp.float32
        anywhere = pl.BlockSpec(memory_space=pl.ANY)
        return pl.pallas_call(
            functools.partial(_kernel, n, heads, kv),
            out_shape=pltpu.VMEM((rows, width), bf16),
            in_specs=[anywhere] * 7,
            out_specs=pl.BlockSpec(memory_space=pltpu.VMEM),
            scratch_shapes=[
                pltpu.VMEM((tokens, width), bf16),
                pltpu.VMEM((rows, width), bf16),
                pltpu.VMEM((heads + 2 * kv, tokens, HEAD), bf16),
                pltpu.VMEM((2, 2, spans, half, span), bf16),
                pltpu.VMEM((2, 3, spans, half, span), bf16),
                pltpu.VMEM((rows, span), f32),
                pltpu.VMEM((SLOTS, PIECES, depth, TILE), bf16),
                pltpu.VMEM((2, tokens, HEAD), f32),
                pltpu.VMEM((width // HEAD, HEAD), bf16),
                pltpu.VMEM((1, width), f32),
                pltpu.VMEM((strips, 2 * half), f32),
                pltpu.VMEM((strips, HEAD + 8, 2 * half), f32),
                pltpu.SemaphoreType.DMA((2, 3, 2)),
                pltpu.SemaphoreType.DMA((2, 3, 2)),
                pltpu.SemaphoreType.DMA((2, 3, spans)),
                pltpu.SemaphoreType.DMA((2, 3, spans)),
                pltpu.SemaphoreType.DMA((SLOTS,)),
                pltpu.SemaphoreType.DMA((4,)),
                pltpu.SemaphoreType.DMA((2,)),
            ],
            compiler_params=pltpu.CompilerParams(collective_id=0, has_side_effects=True, vmem_limit_bytes=VMEM),
        )(x, gain.reshape(width // HEAD, HEAD), _turns(tokens), wq.reshape(PIECES, depth, inner), wk.reshape(PIECES, depth, kv_inner),
          wv.reshape(PIECES, depth, kv_inner), wo)

    tokens, columns = P(("dp", "tp"), None), P(None, "tp")
    return jax.shard_map(
        step,
        mesh=mesh,
        in_specs=(tokens, P(None), columns, columns, columns, P("tp", None)),
        out_specs=tokens,
        check_vma=False,
    )
```

```python
import functools

import jax
import jax.numpy as jnp
import numpy as np
from jax import lax
from jax.experimental import pallas as pl
from jax.experimental.pallas import tpu as pltpu
from jax.sharding import PartitionSpec as P

HEAD = 128
THETA = 10000
NEG = -1e30
HIDDEN = 2 * NEG
LOG2E = 1.4426950408889634
VMEM = 63_000_000
MESH = pl.DeviceIdType.MESH

TILE = 256
PIECES = 4
SLOTS = 3
KEYS = 256
FIRST, PASSED, SECOND = 0, 1, 2
OWN, VIA, SUM = 0, 1, 2


def _dot(a, b, ca=1, cb=0):
    return lax.dot_general(a, b, (((ca,), (cb,)), ((), ())), preferred_element_type=jnp.float32)


def _kernel(n, heads, kv, x_ref, gain_ref, turn_ref, wq_ref, wk_ref, wv_ref, wo_ref, y_ref,
            xs, nb, qkv, sends, recvs, own, wbuf, turn, gain_in, gain, top_s, mix_s,
            ag_send, ag_recv, rs_send, rs_recv, wsem, lsem):
    me = lax.axis_index("tp")
    right, left, far = lax.rem(me + 1, n), lax.rem(me + n - 1, n), lax.rem(me + 2, n)
    sides = ((right, left), (left, right))
    rows, width = x_ref.shape
    half, sub = rows // 2, rows // 4
    group = heads // kv
    inner = heads * HEAD
    depth = width // PIECES
    q_tiles = inner // TILE
    span = PIECES * TILE
    spans = width // span

    load_turn = pltpu.make_async_copy(turn_ref, turn, lsem.at[0])
    load_gain = pltpu.make_async_copy(gain_ref, gain_in, lsem.at[1])

    load_x = pltpu.make_async_copy(x_ref, xs.at[pl.ds(pl.multiple_of(me * rows, rows), rows)], lsem.at[2])


    def fetch_q(j, slot):
        @pl.when(j < q_tiles)
        def _():
            at = pl.ds(pl.multiple_of(j * TILE, TILE), TILE)
            pltpu.make_async_copy(wq_ref.at[:, :, at], wbuf.at[slot], wsem.at[slot]).start()

        @pl.when(j == q_tiles)
        def _():
            pltpu.make_async_copy(wk_ref, wbuf.at[slot], wsem.at[slot]).start()

        @pl.when(j == q_tiles + 1)
        def _():
            pltpu.make_async_copy(wv_ref, wbuf.at[slot], wsem.at[slot]).start()

    def fetch_o(j, slot):
        for c in range(PIECES):
            at = pl.ds(pl.multiple_of(j * span + c * TILE, TILE), TILE)
            pltpu.make_async_copy(wo_ref.at[:, at], wbuf.at[slot, c], wsem.at[slot]).start()

    passes = (fetch_q, fetch_q, fetch_q, fetch_o, fetch_q, fetch_o, fetch_o, fetch_o)
    lengths = [q_tiles + 2 if f is fetch_q else spans for f in passes]

    def stream(index, body):
        fetch, length, before = passes[index], lengths[index], sum(lengths[:index])

        @pl.loop(0, length)
        def _(j):
            slot = lax.rem(before + j, SLOTS)
            pltpu.make_async_copy(wk_ref, wbuf.at[slot], wsem.at[slot]).wait()
            body(j, slot)

            @pl.when(j + SLOTS < length)
            def _():
                fetch(j + SLOTS, slot)

            if index + 1 < len(passes):
                @pl.when(j + SLOTS >= length)
                def _():
                    passes[index + 1](j + SLOTS - length, slot)

    def gathered(way, kind):
        source = sides[way][1]
        near = source * rows + way * half
        return pl.multiple_of(jnp.where(kind == PASSED, far * rows + way * half,
                                        jnp.where(kind == SECOND, source * rows + (1 - way) * half, near)), half)

    def arrival(way, kind, s):
        here = xs.at[pl.ds(pl.multiple_of(gathered(way, kind) + s * sub, sub), sub)]
        return pltpu.make_async_remote_copy(here, here, ag_send.at[way, kind, s], ag_recv.at[way, kind, s],
                                            device_id={"tp": sides[way][1]}, device_id_type=MESH)

    def gather(way, kind, s):
        if kind == PASSED:
            at = gathered(way, FIRST) + s * sub
            source = xs.at[pl.ds(pl.multiple_of(at, sub), sub)]
        else:
            place = (way if kind == FIRST else 1 - way) * half + s * sub
            at = me * rows + place
            source = x_ref.at[pl.ds(place, sub)]
        return pltpu.make_async_remote_copy(source, xs.at[pl.ds(pl.multiple_of(at, sub), sub)], ag_send.at[way, kind, s], ag_recv.at[way, kind, s],
                                            device_id={"tp": sides[way][0]}, device_id_type=MESH)

    def scatter(way, kind, buffer, turn_no, j):
        return pltpu.make_async_remote_copy(sends.at[way, buffer, j], recvs.at[way, kind, j], rs_send.at[way, turn_no, j],
                                            rs_recv.at[way, kind, j], device_id={"tp": sides[way][0]}, device_id_type=MESH)

    def project(index, places):
        for p, place in enumerate(places):
            @pl.loop(0, half // 16)
            def _(i):
                here = pl.ds(pl.multiple_of(place + i * 16, 16), 16)
                there = pl.ds(pl.multiple_of(p * half + i * 16, 16), 16)
                squares = jnp.zeros((16, span), jnp.float32)
                for c in range(spans):
                    wide = xs[here, c * span : (c + 1) * span].astype(jnp.float32)
                    squares += wide * wide
                scale = lax.rsqrt(jnp.sum(squares, -1, keepdims=True) * (1 / width) + 1e-6)
                for c in range(spans):
                    wide = xs[here, c * span : (c + 1) * span].astype(jnp.float32)
                    nb[there, c * span : (c + 1) * span] = (wide * scale * gain[:, c * span : (c + 1) * span]).astype(jnp.bfloat16)

        def body(j, slot):
            t = _dot(nb[:, :depth], wbuf[slot, 0])
            for c in range(1, PIECES):
                t += _dot(nb[:, c * depth : (c + 1) * depth], wbuf[slot, c])
            t = t.astype(jnp.bfloat16)
            for p, place in enumerate(places):
                here = pl.ds(place, half)
                for h in range(TILE // HEAD):
                    head = t[p * half : (p + 1) * half, h * HEAD : (h + 1) * HEAD]

                    @pl.when(j <= q_tiles)
                    def _():
                        wide = head.astype(jnp.float32)
                        turned = wide * turn[0, here, :] + pltpu.roll(wide, HEAD // 2, 1) * turn[1, here, :]
                        qkv[j * (TILE // HEAD) + h, here, :] = turned.astype(jnp.bfloat16)

                    @pl.when(j > q_tiles)
                    def _():
                        qkv[j * (TILE // HEAD) + h, here, :] = head

        stream(index, body)

    strips = [(g, list(range(g * group + i, min(g * group + i + 2, (g + 1) * group)))) for g in range(kv) for i in range(0, group, 2)]

    def attend(places):
        e = HEAD**-0.5 * LOG2E
        ones = jnp.ones((8, KEYS), jnp.bfloat16)

        @pl.loop(0, len(places))
        def _(unit):
            place = pl.multiple_of(jnp.where(unit == 0, places[0], places[1]), half)
            mine = pl.ds(place, half)
            top_s[...] = jnp.full(top_s.shape, NEG, jnp.float32)
            mix_s[...] = jnp.zeros(mix_s.shape, jnp.float32)

            def block(j, masked):
                here = pl.ds(pl.multiple_of(j * KEYS, KEYS), KEYS)
                scores, weights, keeps = [], [], []
                for g, hs in strips:
                    q = jnp.concatenate([qkv[h, mine, :] for h in hs], axis=0)
                    scores.append(_dot(qkv[heads + g, here, :], q, 1, 1))
                if masked:
                    shape = (KEYS, 2 * half)
                    gap = lax.rem(lax.broadcasted_iota(jnp.int32, shape, 1), half) - lax.broadcasted_iota(jnp.int32, shape, 0)
                    ok = gap >= j * KEYS - place
                for i, s in enumerate(scores):
                    wide = s.shape[1]
                    if masked:
                        s = jnp.where(ok[:, :wide], s, HIDDEN)
                    old = top_s[i : i + 1, :wide]
                    top = jnp.maximum(old, s.max(axis=0, keepdims=True))
                    top_s[i : i + 1, :wide] = top
                    weights.append(jnp.exp2((s - top) * e).astype(jnp.bfloat16))
                    keeps.append(jnp.exp2((old - top) * e))
                for i, (g, hs) in enumerate(strips):
                    wide = len(hs) * half
                    values = jnp.concatenate([qkv[heads + kv + g, here, :].T, ones], axis=0)
                    mix_s[i, :, :wide] = mix_s[i, :, :wide] * keeps[i] + _dot(values, weights[i])

            whole = lax.div(place, KEYS)

            @pl.loop(0, whole)
            def _(j):
                block(j, False)

            block(whole, True)
            for i, (g, hs) in enumerate(strips):
                wide = len(hs) * half
                out = (mix_s[i, :HEAD, :wide] * (1 / mix_s[i, HEAD : HEAD + 1, :wide])).T.astype(jnp.bfloat16)
                for m, h in enumerate(hs):
                    qkv[h, mine, :] = out[m * half : (m + 1) * half, :]

    def terms(index, places, before, emit):
        for p, place in enumerate(places):
            for h in range(heads):
                nb[p * half : (p + 1) * half, h * HEAD : (h + 1) * HEAD] = qkv[h, pl.ds(place, half), :]

        def body(j, slot):
            before(j)
            for c in range(PIECES):
                emit(j, slice(c * TILE, (c + 1) * TILE), _dot(nb[:, :inner], wbuf[slot, c]))

        stream(index, body)

    def send_terms(index, places, kinds, turn_no):
        buffer = turn_no % 2

        def before(j):
            @pl.when(j > 0)
            def _():
                for way in range(2):
                    scatter(way, kinds[way], buffer, turn_no, j - 1).start()

            if turn_no == 2:
                for way in range(2):
                    scatter(way, OWN, buffer, 0, j).wait_send()
                    scatter(way, VIA, buffer, turn_no, j).wait_recv()

        def emit(j, columns, t):
            for way in range(2):
                mine = t[way * half : (way + 1) * half]
                if turn_no == 2:
                    mine += recvs[way, VIA, j, :, columns].astype(jnp.float32)
                sends[way, buffer, j, :, columns] = mine.astype(jnp.bfloat16)

        terms(index, places, before, emit)
        for way in range(2):
            scatter(way, kinds[way], buffer, turn_no, spans - 1).start()

    barrier = pltpu.get_barrier_semaphore()
    for other in (left, right):
        pl.semaphore_signal(barrier, inc=1, device_id={"tp": other}, device_id_type=MESH)
    pl.semaphore_wait(barrier, 2)

    pass_first = (me > 0, me == n - 1)
    for s in range(2):
        for way in range(2):
            gather(way, FIRST, s).start()
    load_x.start()
    load_gain.start()
    for j in range(SLOTS):
        passes[0](jnp.int32(j), j)
    load_turn.start()
    for s in range(2):
        for way in range(2):
            @pl.when(jnp.logical_not(pass_first[way]))
            def _():
                gather(way, SECOND, s).start()

    qkv[heads:] = jnp.zeros((2 * kv, *qkv.shape[1:]), jnp.bfloat16)
    load_x.wait()
    load_gain.wait()
    load_turn.wait()
    wide_gain = gain_in[...].astype(jnp.float32)
    for i in range(width // HEAD):
        gain[:, i * HEAD : (i + 1) * HEAD] = wide_gain[i : i + 1, :]
    project(0, (pl.multiple_of(me * rows, rows), pl.multiple_of(me * rows + half, half)))
    for s in range(2):
        for way in range(2):
            arrival(way, FIRST, s).wait_recv()
            gather(way, PASSED, s).start()
    for s in range(2):
        for way in range(2):
            @pl.when(pass_first[way])
            def _():
                gather(way, SECOND, s).start()
    project(1, (gathered(0, FIRST), gathered(1, FIRST)))

    second = (jnp.where(left > 0, PASSED, SECOND), jnp.where(right == n - 1, PASSED, SECOND))
    third = tuple(PASSED + SECOND - kind for kind in second)
    for index, kinds in ((2, second), (4, third)):
        for s in range(2):
            for way in range(2):
                arrival(way, kinds[way], s).wait_recv()
        project(index, (gathered(0, kinds[0]), gathered(1, kinds[1])))

        def scattered(way, kind):
            to = sides[way][0]
            return pl.multiple_of(jnp.where(kind == VIA, far * rows + (1 - way) * half,
                                            jnp.where(kind == OWN, to * rows + way * half, to * rows + (1 - way) * half)), half)

        early = tuple(jnp.where(sides[way][0] < far, OWN, VIA) for way in range(2))
        late = tuple(OWN + VIA - kind for kind in early)
        kinds = early if index == 2 else late
        places = tuple(scattered(way, kinds[way]) for way in range(2))
        attend(places)
        send_terms(index + 1, places, kinds, 0 if index == 2 else 1)

    kinds = (SUM, SUM)
    places = tuple(scattered(way, SUM) for way in range(2))
    attend(places)
    send_terms(6, places, kinds, 2)

    places = (pl.multiple_of(me * rows, rows), pl.multiple_of(me * rows + half, half))
    attend(places)

    def finish(j, columns, t):
        own[:, columns] = t
        if columns.stop < span:
            return
        at = pl.ds(pl.multiple_of(j * span, span), span)
        halves = (slice(0, half), slice(half, rows))
        for p in range(2):
            scatter(p, OWN, 0, 2, j).wait_recv()
            x_part = xs[pl.ds(pl.multiple_of(places[p], half), half), at].astype(jnp.float32)
            own[halves[p], :] = own[halves[p], :] + x_part + recvs[p, OWN, j].astype(jnp.float32)

        @pl.when(j > 0)
        def _():
            for way in range(2):
                scatter(way, SUM, 0, 2, j - 1).wait_send()

        for p in (1, 0):
            scatter(1 - p, SUM, 0, 2, j).wait_recv()
            y_ref[halves[p], at] = (own[halves[p], :] + recvs[1 - p, SUM, j].astype(jnp.float32)).astype(jnp.bfloat16)

    for way in range(2):
        for kind in (FIRST, PASSED, SECOND):
            for s in range(2):
                gather(way, kind, s).wait_send()

    @pl.loop(0, spans)
    def _(j):
        for way in range(2):
            scatter(way, late[way], 1, 1, j).wait_send()

    terms(7, places, lambda j: None, finish)
    for way in range(2):
        scatter(way, SUM, 0, 2, spans - 1).wait_send()


def _turns(tokens):
    half = HEAD // 2
    angle = np.arange(tokens, dtype=np.float32)[:, None] * np.float32(THETA) ** (-np.arange(half, dtype=np.float32) / np.float32(half))
    cos, sin = np.cos(angle.astype(np.float64)), np.sin(angle.astype(np.float64))
    return np.stack([np.concatenate([cos, cos], -1), np.concatenate([-sin, sin], -1)]).astype(np.float32)


def solution(mesh):
    n = mesh.shape["tp"]

    def step(x, gain, wq, wk, wv, wo):
        rows, width = x.shape
        inner, kv_inner = wq.shape[1], wk.shape[1]
        heads, kv = inner // HEAD, kv_inner // HEAD
        half, tokens, span = rows // 2, n * rows, PIECES * TILE
        spans, depth = width // span, width // PIECES
        strips = kv * -(-(heads // kv) // 2)
        bf16, f32 = jnp.bfloat16, jnp.float32
        anywhere = pl.BlockSpec(memory_space=pl.ANY)
        return pl.pallas_call(
            functools.partial(_kernel, n, heads, kv),
            out_shape=pltpu.VMEM((rows, width), bf16),
            in_specs=[anywhere] * 7,
            out_specs=pl.BlockSpec(memory_space=pltpu.VMEM),
            scratch_shapes=[
                pltpu.VMEM((tokens, width), bf16),
                pltpu.VMEM((rows, width), bf16),
                pltpu.VMEM((heads + 2 * kv, tokens, HEAD), bf16),
                pltpu.VMEM((2, 2, spans, half, span), bf16),
                pltpu.VMEM((2, 3, spans, half, span), bf16),
                pltpu.VMEM((rows, span), f32),
                pltpu.VMEM((SLOTS, PIECES, depth, TILE), bf16),
                pltpu.VMEM((2, tokens, HEAD), f32),
                pltpu.VMEM((width // HEAD, HEAD), bf16),
                pltpu.VMEM((1, width), f32),
                pltpu.VMEM((strips, 2 * half), f32),
                pltpu.VMEM((strips, HEAD + 8, 2 * half), f32),
                pltpu.SemaphoreType.DMA((2, 3, 2)),
                pltpu.SemaphoreType.DMA((2, 3, 2)),
                pltpu.SemaphoreType.DMA((2, 3, spans)),
                pltpu.SemaphoreType.DMA((2, 3, spans)),
                pltpu.SemaphoreType.DMA((SLOTS,)),
                pltpu.SemaphoreType.DMA((3,)),
            ],
            compiler_params=pltpu.CompilerParams(collective_id=0, has_side_effects=True, vmem_limit_bytes=VMEM),
        )(x, gain.reshape(width // HEAD, HEAD), _turns(tokens), wq.reshape(PIECES, depth, inner), wk.reshape(PIECES, depth, kv_inner),
          wv.reshape(PIECES, depth, kv_inner), wo)

    tokens, columns = P(("dp", "tp"), None), P(None, "tp")
    return jax.shard_map(
        step,
        mesh=mesh,
        in_specs=(tokens, P(None), columns, columns, columns, P("tp", None)),
        out_specs=tokens,
        check_vma=False,
    )
```

```python
import functools

import jax
import jax.numpy as jnp
import numpy as np
from jax import lax
from jax.experimental import pallas as pl
from jax.experimental.pallas import tpu as pltpu
from jax.sharding import PartitionSpec as P

HEAD = 128
THETA = 10000
NEG = -1e30
HIDDEN = 2 * NEG
LOG2E = 1.4426950408889634
VMEM = 63_000_000
MESH = pl.DeviceIdType.MESH

TILE = 256
PIECES = 4
SLOTS = 3
KEYS = 256
FIRST, PASSED, SECOND = 0, 1, 2
OWN, VIA, SUM = 0, 1, 2


def _dot(a, b, ca=1, cb=0):
    return lax.dot_general(a, b, (((ca,), (cb,)), ((), ())), preferred_element_type=jnp.float32)


def _kernel(n, heads, kv, x_ref, gain_ref, turn_ref, wq_ref, wk_ref, wv_ref, wo_ref, y_ref,
            xs, nb, qkv, sends, recvs, own, wbuf, turn, gain_in, gain, top_s, mix_s,
            ag_send, ag_recv, rs_send, rs_recv, wsem, xsem, lsem):
    me = lax.axis_index("tp")
    right, left, far = lax.rem(me + 1, n), lax.rem(me + n - 1, n), lax.rem(me + 2, n)
    sides = ((right, left), (left, right))
    rows, width = x_ref.shape
    half, sub = rows // 2, rows // 4
    group = heads // kv
    inner = heads * HEAD
    depth = width // PIECES
    q_tiles = inner // TILE
    span = PIECES * TILE
    spans = width // span

    lead = 16
    parts = {FIRST: ((0, lead), (lead, sub - lead), (sub, sub)), PASSED: ((0, sub), (sub, sub)), SECOND: ((0, sub), (sub, sub))}

    load_turn = pltpu.make_async_copy(turn_ref, turn, lsem.at[0])
    load_gain = pltpu.make_async_copy(gain_ref, gain_in, lsem.at[1])

    def load_x(h, start, count):
        place = h * half + start
        here = xs.at[pl.ds(pl.multiple_of(me * rows + place, lead), count)]
        return pltpu.make_async_copy(x_ref.at[pl.ds(place, count)], here, xsem.at[h, min(start, 1)])


    def fetch_q(j, slot):
        @pl.when(j < q_tiles)
        def _():
            at = pl.ds(pl.multiple_of(j * TILE, TILE), TILE)
            pltpu.make_async_copy(wq_ref.at[:, :, at], wbuf.at[slot], wsem.at[slot]).start()

        @pl.when(j == q_tiles)
        def _():
            pltpu.make_async_copy(wk_ref, wbuf.at[slot], wsem.at[slot]).start()

        @pl.when(j == q_tiles + 1)
        def _():
            pltpu.make_async_copy(wv_ref, wbuf.at[slot], wsem.at[slot]).start()

    def fetch_o(j, slot):
        for c in range(PIECES):
            at = pl.ds(pl.multiple_of(j * span + c * TILE, TILE), TILE)
            pltpu.make_async_copy(wo_ref.at[:, at], wbuf.at[slot, c], wsem.at[slot]).start()

    passes = (fetch_q, fetch_q, fetch_q, fetch_o, fetch_q, fetch_o, fetch_o, fetch_o)
    lengths = [q_tiles + 2 if f is fetch_q else spans for f in passes]

    def stream(index, body):
        fetch, length, before = passes[index], lengths[index], sum(lengths[:index])

        @pl.loop(0, length)
        def _(j):
            slot = lax.rem(before + j, SLOTS)
            pltpu.make_async_copy(wk_ref, wbuf.at[slot], wsem.at[slot]).wait()
            body(j, slot)

            @pl.when(j + SLOTS < length)
            def _():
                fetch(j + SLOTS, slot)

            if index + 1 < len(passes):
                @pl.when(j + SLOTS >= length)
                def _():
                    passes[index + 1](j + SLOTS - length, slot)

    def gathered(way, kind):
        source = sides[way][1]
        near = source * rows + way * half
        return pl.multiple_of(jnp.where(kind == PASSED, far * rows + way * half,
                                        jnp.where(kind == SECOND, source * rows + (1 - way) * half, near)), half)

    def arrival(way, kind, s):
        start, count = parts[SECOND][s] if kind is not FIRST else parts[FIRST][s]
        here = xs.at[pl.ds(pl.multiple_of(gathered(way, kind) + start, lead), count)]
        return pltpu.make_async_remote_copy(here, here, ag_send.at[way, kind, s], ag_recv.at[way, kind, s],
                                            device_id={"tp": sides[way][1]}, device_id_type=MESH)

    def gather(way, kind, s):
        start, count = parts[kind][s]
        if kind == PASSED:
            at = gathered(way, FIRST) + start
            source = xs.at[pl.ds(pl.multiple_of(at, lead), count)]
        else:
            place = (way if kind == FIRST else 1 - way) * half + start
            at = me * rows + place
            source = x_ref.at[pl.ds(place, count)]
            if kind == FIRST and s == 0:
                source = xs.at[pl.ds(pl.multiple_of(at, lead), count)]
        return pltpu.make_async_remote_copy(source, xs.at[pl.ds(pl.multiple_of(at, lead), count)], ag_send.at[way, kind, s],
                                            ag_recv.at[way, kind, s], device_id={"tp": sides[way][0]}, device_id_type=MESH)

    def scatter(way, kind, buffer, turn_no, j):
        return pltpu.make_async_remote_copy(sends.at[way, buffer, j], recvs.at[way, kind, j], rs_send.at[way, turn_no, j],
                                            rs_recv.at[way, kind, j], device_id={"tp": sides[way][0]}, device_id_type=MESH)

    def project(index, places):
        for p, place in enumerate(places):
            @pl.loop(0, half // 16)
            def _(i):
                here = pl.ds(pl.multiple_of(place + i * 16, 16), 16)
                there = pl.ds(pl.multiple_of(p * half + i * 16, 16), 16)
                squares = jnp.zeros((16, span), jnp.float32)
                for c in range(spans):
                    wide = xs[here, c * span : (c + 1) * span].astype(jnp.float32)
                    squares += wide * wide
                scale = lax.rsqrt(jnp.sum(squares, -1, keepdims=True) * (1 / width) + 1e-6)
                for c in range(spans):
                    wide = xs[here, c * span : (c + 1) * span].astype(jnp.float32)
                    nb[there, c * span : (c + 1) * span] = (wide * scale * gain[:, c * span : (c + 1) * span]).astype(jnp.bfloat16)

        def body(j, slot):
            t = _dot(nb[:, :depth], wbuf[slot, 0])
            for c in range(1, PIECES):
                t += _dot(nb[:, c * depth : (c + 1) * depth], wbuf[slot, c])
            t = t.astype(jnp.bfloat16)
            for p, place in enumerate(places):
                here = pl.ds(place, half)
                for h in range(TILE // HEAD):
                    head = t[p * half : (p + 1) * half, h * HEAD : (h + 1) * HEAD]

                    @pl.when(j <= q_tiles)
                    def _():
                        wide = head.astype(jnp.float32)
                        turned = wide * turn[0, here, :] + pltpu.roll(wide, HEAD // 2, 1) * turn[1, here, :]
                        qkv[j * (TILE // HEAD) + h, here, :] = turned.astype(jnp.bfloat16)

                    @pl.when(j > q_tiles)
                    def _():
                        qkv[j * (TILE // HEAD) + h, here, :] = head

        stream(index, body)

    strips = [(g, list(range(g * group + i, min(g * group + i + 2, (g + 1) * group)))) for g in range(kv) for i in range(0, group, 2)]

    def attend(places):
        e = HEAD**-0.5 * LOG2E
        ones = jnp.ones((8, KEYS), jnp.bfloat16)

        @pl.loop(0, len(places))
        def _(unit):
            place = pl.multiple_of(jnp.where(unit == 0, places[0], places[1]), half)
            mine = pl.ds(place, half)
            top_s[...] = jnp.full(top_s.shape, NEG, jnp.float32)
            mix_s[...] = jnp.zeros(mix_s.shape, jnp.float32)

            def block(j, masked):
                here = pl.ds(pl.multiple_of(j * KEYS, KEYS), KEYS)
                scores, weights, keeps = [], [], []
                for g, hs in strips:
                    q = jnp.concatenate([qkv[h, mine, :] for h in hs], axis=0)
                    scores.append(_dot(qkv[heads + g, here, :], q, 1, 1))
                if masked:
                    shape = (KEYS, 2 * half)
                    gap = lax.rem(lax.broadcasted_iota(jnp.int32, shape, 1), half) - lax.broadcasted_iota(jnp.int32, shape, 0)
                    ok = gap >= j * KEYS - place
                for i, s in enumerate(scores):
                    wide = s.shape[1]
                    if masked:
                        s = jnp.where(ok[:, :wide], s, HIDDEN)
                    old = top_s[i : i + 1, :wide]
                    top = jnp.maximum(old, s.max(axis=0, keepdims=True))
                    top_s[i : i + 1, :wide] = top
                    weights.append(jnp.exp2((s - top) * e).astype(jnp.bfloat16))
                    keeps.append(jnp.exp2((old - top) * e))
                for i, (g, hs) in enumerate(strips):
                    wide = len(hs) * half
                    values = jnp.concatenate([qkv[heads + kv + g, here, :].T, ones], axis=0)
                    mix_s[i, :, :wide] = mix_s[i, :, :wide] * keeps[i] + _dot(values, weights[i])

            whole = lax.div(place, KEYS)

            @pl.loop(0, whole)
            def _(j):
                block(j, False)

            block(whole, True)
            for i, (g, hs) in enumerate(strips):
                wide = len(hs) * half
                out = (mix_s[i, :HEAD, :wide] * (1 / mix_s[i, HEAD : HEAD + 1, :wide])).T.astype(jnp.bfloat16)
                for m, h in enumerate(hs):
                    qkv[h, mine, :] = out[m * half : (m + 1) * half, :]

    def terms(index, places, before, emit):
        for p, place in enumerate(places):
            for h in range(heads):
                nb[p * half : (p + 1) * half, h * HEAD : (h + 1) * HEAD] = qkv[h, pl.ds(place, half), :]

        def body(j, slot):
            before(j)
            for c in range(PIECES):
                emit(j, slice(c * TILE, (c + 1) * TILE), _dot(nb[:, :inner], wbuf[slot, c]))

        stream(index, body)

    def send_terms(index, places, kinds, turn_no):
        buffer = turn_no % 2

        def before(j):
            @pl.when(j > 0)
            def _():
                for way in range(2):
                    scatter(way, kinds[way], buffer, turn_no, j - 1).start()

            if turn_no == 2:
                for way in range(2):
                    scatter(way, OWN, buffer, 0, j).wait_send()
                    scatter(way, VIA, buffer, turn_no, j).wait_recv()

        def emit(j, columns, t):
            for way in range(2):
                mine = t[way * half : (way + 1) * half]
                if turn_no == 2:
                    mine += recvs[way, VIA, j, :, columns].astype(jnp.float32)
                sends[way, buffer, j, :, columns] = mine.astype(jnp.bfloat16)

        terms(index, places, before, emit)
        for way in range(2):
            scatter(way, kinds[way], buffer, turn_no, spans - 1).start()

    barrier = pltpu.get_barrier_semaphore()
    for other in (left, right):
        pl.semaphore_signal(barrier, inc=1, device_id={"tp": other}, device_id_type=MESH)
    for way in range(2):
        load_x(way, 0, lead).start()
    pl.semaphore_wait(barrier, 2)

    pass_first = (me > 0, me == n - 1)
    for s in range(3):
        for way in range(2):
            if s == 0:
                load_x(way, 0, lead).wait()
            gather(way, FIRST, s).start()
    for way in range(2):
        load_x(way, lead, half - lead).start()
    load_gain.start()
    for j in range(SLOTS):
        passes[0](jnp.int32(j), j)
    load_turn.start()
    for s in range(2):
        for way in range(2):
            @pl.when(jnp.logical_not(pass_first[way]))
            def _():
                gather(way, SECOND, s).start()

    qkv[heads:] = jnp.zeros((2 * kv, *qkv.shape[1:]), jnp.bfloat16)
    for way in range(2):
        load_x(way, lead, half - lead).wait()
    load_gain.wait()
    load_turn.wait()
    wide_gain = gain_in[...].astype(jnp.float32)
    for i in range(width // HEAD):
        gain[:, i * HEAD : (i + 1) * HEAD] = wide_gain[i : i + 1, :]
    project(0, (pl.multiple_of(me * rows, rows), pl.multiple_of(me * rows + half, half)))
    for s in range(3):
        for way in range(2):
            arrival(way, FIRST, s).wait_recv()
            if s > 0:
                gather(way, PASSED, s - 1).start()
    for s in range(2):
        for way in range(2):
            @pl.when(pass_first[way])
            def _():
                gather(way, SECOND, s).start()
    project(1, (gathered(0, FIRST), gathered(1, FIRST)))

    second = (jnp.where(left > 0, PASSED, SECOND), jnp.where(right == n - 1, PASSED, SECOND))
    third = tuple(PASSED + SECOND - kind for kind in second)
    for index, kinds in ((2, second), (4, third)):
        for s in range(2):
            for way in range(2):
                arrival(way, kinds[way], s).wait_recv()
        project(index, (gathered(0, kinds[0]), gathered(1, kinds[1])))

        def scattered(way, kind):
            to = sides[way][0]
            return pl.multiple_of(jnp.where(kind == VIA, far * rows + (1 - way) * half,
                                            jnp.where(kind == OWN, to * rows + way * half, to * rows + (1 - way) * half)), half)

        early = tuple(jnp.where(sides[way][0] < far, OWN, VIA) for way in range(2))
        late = tuple(OWN + VIA - kind for kind in early)
        kinds = early if index == 2 else late
        places = tuple(scattered(way, kinds[way]) for way in range(2))
        attend(places)
        send_terms(index + 1, places, kinds, 0 if index == 2 else 1)

    kinds = (SUM, SUM)
    places = tuple(scattered(way, SUM) for way in range(2))
    attend(places)
    send_terms(6, places, kinds, 2)

    places = (pl.multiple_of(me * rows, rows), pl.multiple_of(me * rows + half, half))
    attend(places)

    def finish(j, columns, t):
        own[:, columns] = t
        if columns.stop < span:
            return
        at = pl.ds(pl.multiple_of(j * span, span), span)
        halves = (slice(0, half), slice(half, rows))
        for p in range(2):
            scatter(p, OWN, 0, 2, j).wait_recv()
            x_part = xs[pl.ds(pl.multiple_of(places[p], half), half), at].astype(jnp.float32)
            own[halves[p], :] = own[halves[p], :] + x_part + recvs[p, OWN, j].astype(jnp.float32)

        @pl.when(j > 0)
        def _():
            for way in range(2):
                scatter(way, SUM, 0, 2, j - 1).wait_send()

        for p in (1, 0):
            scatter(1 - p, SUM, 0, 2, j).wait_recv()
            y_ref[halves[p], at] = (own[halves[p], :] + recvs[1 - p, SUM, j].astype(jnp.float32)).astype(jnp.bfloat16)

    for way in range(2):
        for kind in (FIRST, PASSED, SECOND):
            for s in range(len(parts[kind])):
                gather(way, kind, s).wait_send()

    @pl.loop(0, spans)
    def _(j):
        for way in range(2):
            scatter(way, late[way], 1, 1, j).wait_send()

    terms(7, places, lambda j: None, finish)
    for way in range(2):
        scatter(way, SUM, 0, 2, spans - 1).wait_send()


def _turns(tokens):
    half = HEAD // 2
    angle = np.arange(tokens, dtype=np.float32)[:, None] * np.float32(THETA) ** (-np.arange(half, dtype=np.float32) / np.float32(half))
    cos, sin = np.cos(angle.astype(np.float64)), np.sin(angle.astype(np.float64))
    return np.stack([np.concatenate([cos, cos], -1), np.concatenate([-sin, sin], -1)]).astype(np.float32)


def solution(mesh):
    n = mesh.shape["tp"]

    def step(x, gain, wq, wk, wv, wo):
        rows, width = x.shape
        inner, kv_inner = wq.shape[1], wk.shape[1]
        heads, kv = inner // HEAD, kv_inner // HEAD
        half, tokens, span = rows // 2, n * rows, PIECES * TILE
        spans, depth = width // span, width // PIECES
        strips = kv * -(-(heads // kv) // 2)
        bf16, f32 = jnp.bfloat16, jnp.float32
        anywhere = pl.BlockSpec(memory_space=pl.ANY)
        return pl.pallas_call(
            functools.partial(_kernel, n, heads, kv),
            out_shape=pltpu.VMEM((rows, width), bf16),
            in_specs=[anywhere] * 7,
            out_specs=pl.BlockSpec(memory_space=pltpu.VMEM),
            scratch_shapes=[
                pltpu.VMEM((tokens, width), bf16),
                pltpu.VMEM((rows, width), bf16),
                pltpu.VMEM((heads + 2 * kv, tokens, HEAD), bf16),
                pltpu.VMEM((2, 2, spans, half, span), bf16),
                pltpu.VMEM((2, 3, spans, half, span), bf16),
                pltpu.VMEM((rows, span), f32),
                pltpu.VMEM((SLOTS, PIECES, depth, TILE), bf16),
                pltpu.VMEM((2, tokens, HEAD), f32),
                pltpu.VMEM((width // HEAD, HEAD), bf16),
                pltpu.VMEM((1, width), f32),
                pltpu.VMEM((strips, 2 * half), f32),
                pltpu.VMEM((strips, HEAD + 8, 2 * half), f32),
                pltpu.SemaphoreType.DMA((2, 3, 3)),
                pltpu.SemaphoreType.DMA((2, 3, 3)),
                pltpu.SemaphoreType.DMA((2, 3, spans)),
                pltpu.SemaphoreType.DMA((2, 3, spans)),
                pltpu.SemaphoreType.DMA((SLOTS,)),
                pltpu.SemaphoreType.DMA((2, 2)),
                pltpu.SemaphoreType.DMA((2,)),
            ],
            compiler_params=pltpu.CompilerParams(collective_id=0, has_side_effects=True, vmem_limit_bytes=VMEM),
        )(x, gain.reshape(width // HEAD, HEAD), _turns(tokens), wq.reshape(PIECES, depth, inner), wk.reshape(PIECES, depth, kv_inner),
          wv.reshape(PIECES, depth, kv_inner), wo)

    tokens, columns = P(("dp", "tp"), None), P(None, "tp")
    return jax.shard_map(
        step,
        mesh=mesh,
        in_specs=(tokens, P(None), columns, columns, columns, P("tp", None)),
        out_specs=tokens,
        check_vma=False,
    )
```

```python
import functools

import jax
import jax.numpy as jnp
import numpy as np
from jax import lax
from jax.experimental import pallas as pl
from jax.experimental.pallas import tpu as pltpu
from jax.sharding import PartitionSpec as P

HEAD = 128
THETA = 10000
NEG = -1e30
HIDDEN = 2 * NEG
LOG2E = 1.4426950408889634
VMEM = 63_000_000
MESH = pl.DeviceIdType.MESH

TILE = 256
PIECES = 4
SLOTS = 3
KEYS = 256
FIRST, PASSED, SECOND = 0, 1, 2
OWN, VIA, SUM = 0, 1, 2


def _dot(a, b, ca=1, cb=0):
    return lax.dot_general(a, b, (((ca,), (cb,)), ((), ())), preferred_element_type=jnp.float32)


def _kernel(n, heads, kv, x_ref, gain_ref, turn_ref, wq_ref, wk_ref, wv_ref, wo_ref, y_ref,
            xs, nb, qkv, sends, recvs, own, wbuf, turn, gain_in, gain, top_s, mix_s,
            ag_send, ag_recv, rs_send, rs_recv, wsem, lsem, here_sem):
    me = lax.axis_index("tp")
    right, left, far = lax.rem(me + 1, n), lax.rem(me + n - 1, n), lax.rem(me + 2, n)
    sides = ((right, left), (left, right))
    rows, width = x_ref.shape
    half, sub = rows // 2, rows // 4
    group = heads // kv
    inner = heads * HEAD
    depth = width // PIECES
    q_tiles = inner // TILE
    span = PIECES * TILE
    spans = width // span

    load_turn = pltpu.make_async_copy(turn_ref, turn, lsem.at[0])
    load_gain = pltpu.make_async_copy(gain_ref, gain_in, lsem.at[1])

    load_x = pltpu.make_async_copy(x_ref, xs.at[pl.ds(pl.multiple_of(me * rows, rows), rows)], lsem.at[2])


    def fetch_q(j, slot):
        @pl.when(j < q_tiles)
        def _():
            at = pl.ds(pl.multiple_of(j * TILE, TILE), TILE)
            pltpu.make_async_copy(wq_ref.at[:, :, at], wbuf.at[slot], wsem.at[slot]).start()

        @pl.when(j == q_tiles)
        def _():
            pltpu.make_async_copy(wk_ref, wbuf.at[slot], wsem.at[slot]).start()

        @pl.when(j == q_tiles + 1)
        def _():
            pltpu.make_async_copy(wv_ref, wbuf.at[slot], wsem.at[slot]).start()

    def fetch_o(j, slot):
        for c in range(PIECES):
            at = pl.ds(pl.multiple_of(j * span + c * TILE, TILE), TILE)
            pltpu.make_async_copy(wo_ref.at[:, at], wbuf.at[slot, c], wsem.at[slot]).start()

    passes = (fetch_q, fetch_q, fetch_q, fetch_o, fetch_q, fetch_o, fetch_o, fetch_o)
    lengths = [q_tiles + 2 if f is fetch_q else spans for f in passes]

    def stream(index, body):
        fetch, length, before = passes[index], lengths[index], sum(lengths[:index])

        @pl.loop(0, length)
        def _(j):
            slot = lax.rem(before + j, SLOTS)
            pltpu.make_async_copy(wk_ref, wbuf.at[slot], wsem.at[slot]).wait()
            body(j, slot)

            @pl.when(j + SLOTS < length)
            def _():
                fetch(j + SLOTS, slot)

            if index + 1 < len(passes):
                @pl.when(j + SLOTS >= length)
                def _():
                    passes[index + 1](j + SLOTS - length, slot)

    def gathered(way, kind):
        source = sides[way][1]
        near = source * rows + way * half
        return pl.multiple_of(jnp.where(kind == PASSED, far * rows + way * half,
                                        jnp.where(kind == SECOND, source * rows + (1 - way) * half, near)), half)

    def arrival(way, kind, s):
        here = xs.at[pl.ds(pl.multiple_of(gathered(way, kind) + s * sub, sub), sub)]
        return pltpu.make_async_remote_copy(here, here, ag_send.at[way, kind, s], ag_recv.at[way, kind, s],
                                            device_id={"tp": sides[way][1]}, device_id_type=MESH)

    def gather(way, kind, s):
        if kind == PASSED:
            at = gathered(way, FIRST) + s * sub
            source = xs.at[pl.ds(pl.multiple_of(at, sub), sub)]
        else:
            place = (way if kind == FIRST else 1 - way) * half + s * sub
            at = me * rows + place
            source = x_ref.at[pl.ds(place, sub)]
        return pltpu.make_async_remote_copy(source, xs.at[pl.ds(pl.multiple_of(at, sub), sub)], ag_send.at[way, kind, s], ag_recv.at[way, kind, s],
                                            device_id={"tp": sides[way][0]}, device_id_type=MESH)

    def scatter(way, kind, buffer, turn_no, j):
        return pltpu.make_async_remote_copy(sends.at[way, buffer, j], recvs.at[way, kind, j], rs_send.at[way, turn_no, j],
                                            rs_recv.at[way, kind, j], device_id={"tp": sides[way][0]}, device_id_type=MESH)

    def project(index, places):
        for p, place in enumerate(places):
            @pl.loop(0, half // 16)
            def _(i):
                here = pl.ds(pl.multiple_of(place + i * 16, 16), 16)
                there = pl.ds(pl.multiple_of(p * half + i * 16, 16), 16)
                squares = jnp.zeros((16, span), jnp.float32)
                for c in range(spans):
                    wide = xs[here, c * span : (c + 1) * span].astype(jnp.float32)
                    squares += wide * wide
                scale = lax.rsqrt(jnp.sum(squares, -1, keepdims=True) * (1 / width) + 1e-6)
                for c in range(spans):
                    wide = xs[here, c * span : (c + 1) * span].astype(jnp.float32)
                    nb[there, c * span : (c + 1) * span] = (wide * scale * gain[:, c * span : (c + 1) * span]).astype(jnp.bfloat16)

        def body(j, slot):
            t = _dot(nb[:, :depth], wbuf[slot, 0])
            for c in range(1, PIECES):
                t += _dot(nb[:, c * depth : (c + 1) * depth], wbuf[slot, c])
            t = t.astype(jnp.bfloat16)
            for p, place in enumerate(places):
                here = pl.ds(place, half)
                for h in range(TILE // HEAD):
                    head = t[p * half : (p + 1) * half, h * HEAD : (h + 1) * HEAD]

                    @pl.when(j <= q_tiles)
                    def _():
                        wide = head.astype(jnp.float32)
                        turned = wide * turn[0, here, :] + pltpu.roll(wide, HEAD // 2, 1) * turn[1, here, :]
                        qkv[j * (TILE // HEAD) + h, here, :] = turned.astype(jnp.bfloat16)

                    @pl.when(j > q_tiles)
                    def _():
                        qkv[j * (TILE // HEAD) + h, here, :] = head

        stream(index, body)

    strips = [(g, list(range(g * group + i, min(g * group + i + 2, (g + 1) * group)))) for g in range(kv) for i in range(0, group, 2)]

    def attend(places):
        e = HEAD**-0.5 * LOG2E
        ones = jnp.ones((8, KEYS), jnp.bfloat16)

        @pl.loop(0, len(places))
        def _(unit):
            place = pl.multiple_of(jnp.where(unit == 0, places[0], places[1]), half)
            mine = pl.ds(place, half)
            top_s[...] = jnp.full(top_s.shape, NEG, jnp.float32)
            mix_s[...] = jnp.zeros(mix_s.shape, jnp.float32)

            def block(j, masked):
                here = pl.ds(pl.multiple_of(j * KEYS, KEYS), KEYS)
                scores, weights, keeps = [], [], []
                for g, hs in strips:
                    q = jnp.concatenate([qkv[h, mine, :] for h in hs], axis=0)
                    scores.append(_dot(qkv[heads + g, here, :], q, 1, 1))
                if masked:
                    shape = (KEYS, 2 * half)
                    gap = lax.rem(lax.broadcasted_iota(jnp.int32, shape, 1), half) - lax.broadcasted_iota(jnp.int32, shape, 0)
                    ok = gap >= j * KEYS - place
                for i, s in enumerate(scores):
                    wide = s.shape[1]
                    if masked:
                        s = jnp.where(ok[:, :wide], s, HIDDEN)
                    old = top_s[i : i + 1, :wide]
                    top = jnp.maximum(old, s.max(axis=0, keepdims=True))
                    top_s[i : i + 1, :wide] = top
                    weights.append(jnp.exp2((s - top) * e).astype(jnp.bfloat16))
                    keeps.append(jnp.exp2((old - top) * e))
                for i, (g, hs) in enumerate(strips):
                    wide = len(hs) * half
                    values = jnp.concatenate([qkv[heads + kv + g, here, :].T, ones], axis=0)
                    mix_s[i, :, :wide] = mix_s[i, :, :wide] * keeps[i] + _dot(values, weights[i])

            whole = lax.div(place, KEYS)

            @pl.loop(0, whole)
            def _(j):
                block(j, False)

            block(whole, True)
            for i, (g, hs) in enumerate(strips):
                wide = len(hs) * half
                out = (mix_s[i, :HEAD, :wide] * (1 / mix_s[i, HEAD : HEAD + 1, :wide])).T.astype(jnp.bfloat16)
                for m, h in enumerate(hs):
                    qkv[h, mine, :] = out[m * half : (m + 1) * half, :]

    def terms(index, places, before, emit):
        for p, place in enumerate(places):
            for h in range(heads):
                nb[p * half : (p + 1) * half, h * HEAD : (h + 1) * HEAD] = qkv[h, pl.ds(place, half), :]

        def body(j, slot):
            before(j)
            for c in range(PIECES):
                emit(j, slice(c * TILE, (c + 1) * TILE), _dot(nb[:, :inner], wbuf[slot, c]))

        stream(index, body)

    def send_terms(index, places, kinds, turn_no):
        buffer = turn_no % 2

        def before(j):
            @pl.when(j > 0)
            def _():
                for way in range(2):
                    scatter(way, kinds[way], buffer, turn_no, j - 1).start()

            if turn_no == 2:
                for way in range(2):
                    scatter(way, OWN, buffer, 0, j).wait_send()
                    scatter(way, VIA, buffer, turn_no, j).wait_recv()

        def emit(j, columns, t):
            for way in range(2):
                mine = t[way * half : (way + 1) * half]
                if turn_no == 2:
                    mine += recvs[way, VIA, j, :, columns].astype(jnp.float32)
                sends[way, buffer, j, :, columns] = mine.astype(jnp.bfloat16)

        terms(index, places, before, emit)
        for way in range(2):
            scatter(way, kinds[way], buffer, turn_no, spans - 1).start()

    barrier = pltpu.get_barrier_semaphore()
    pl.semaphore_signal(barrier, inc=1, device_id={"tp": left}, device_id_type=MESH)
    pl.semaphore_wait(barrier, 1)
    pl.semaphore_signal(here_sem, inc=1, device_id={"tp": right}, device_id_type=MESH)
    pass_first = (me > 0, me == n - 1)
    for way in range(2):
        if way == 1:
            pl.semaphore_wait(here_sem, 1)
        for s in range(2):
            gather(way, FIRST, s).start()
    load_x.start()
    load_gain.start()
    for j in range(SLOTS):
        passes[0](jnp.int32(j), j)
    load_turn.start()
    for s in range(2):
        for way in range(2):
            @pl.when(jnp.logical_not(pass_first[way]))
            def _():
                gather(way, SECOND, s).start()

    qkv[heads:] = jnp.zeros((2 * kv, *qkv.shape[1:]), jnp.bfloat16)
    load_x.wait()
    load_gain.wait()
    load_turn.wait()
    wide_gain = gain_in[...].astype(jnp.float32)
    for i in range(width // HEAD):
        gain[:, i * HEAD : (i + 1) * HEAD] = wide_gain[i : i + 1, :]
    project(0, (pl.multiple_of(me * rows, rows), pl.multiple_of(me * rows + half, half)))
    for s in range(2):
        for way in range(2):
            arrival(way, FIRST, s).wait_recv()
            gather(way, PASSED, s).start()
    for s in range(2):
        for way in range(2):
            @pl.when(pass_first[way])
            def _():
                gather(way, SECOND, s).start()
    project(1, (gathered(0, FIRST), gathered(1, FIRST)))

    second = (jnp.where(left > 0, PASSED, SECOND), jnp.where(right == n - 1, PASSED, SECOND))
    third = tuple(PASSED + SECOND - kind for kind in second)
    for index, kinds in ((2, second), (4, third)):
        for s in range(2):
            for way in range(2):
                arrival(way, kinds[way], s).wait_recv()
        project(index, (gathered(0, kinds[0]), gathered(1, kinds[1])))

        def scattered(way, kind):
            to = sides[way][0]
            return pl.multiple_of(jnp.where(kind == VIA, far * rows + (1 - way) * half,
                                            jnp.where(kind == OWN, to * rows + way * half, to * rows + (1 - way) * half)), half)

        early = tuple(jnp.where(sides[way][0] < far, OWN, VIA) for way in range(2))
        late = tuple(OWN + VIA - kind for kind in early)
        kinds = early if index == 2 else late
        places = tuple(scattered(way, kinds[way]) for way in range(2))
        attend(places)
        send_terms(index + 1, places, kinds, 0 if index == 2 else 1)

    kinds = (SUM, SUM)
    places = tuple(scattered(way, SUM) for way in range(2))
    attend(places)
    send_terms(6, places, kinds, 2)

    places = (pl.multiple_of(me * rows, rows), pl.multiple_of(me * rows + half, half))
    attend(places)

    def finish(j, columns, t):
        own[:, columns] = t
        if columns.stop < span:
            return
        at = pl.ds(pl.multiple_of(j * span, span), span)
        halves = (slice(0, half), slice(half, rows))
        for p in range(2):
            scatter(p, OWN, 0, 2, j).wait_recv()
            x_part = xs[pl.ds(pl.multiple_of(places[p], half), half), at].astype(jnp.float32)
            own[halves[p], :] = own[halves[p], :] + x_part + recvs[p, OWN, j].astype(jnp.float32)

        @pl.when(j > 0)
        def _():
            for way in range(2):
                scatter(way, SUM, 0, 2, j - 1).wait_send()

        for p in (1, 0):
            scatter(1 - p, SUM, 0, 2, j).wait_recv()
            y_ref[halves[p], at] = (own[halves[p], :] + recvs[1 - p, SUM, j].astype(jnp.float32)).astype(jnp.bfloat16)

    for way in range(2):
        for kind in (FIRST, PASSED, SECOND):
            for s in range(2):
                gather(way, kind, s).wait_send()

    @pl.loop(0, spans)
    def _(j):
        for way in range(2):
            scatter(way, late[way], 1, 1, j).wait_send()

    terms(7, places, lambda j: None, finish)
    for way in range(2):
        scatter(way, SUM, 0, 2, spans - 1).wait_send()


def _turns(tokens):
    half = HEAD // 2
    angle = np.arange(tokens, dtype=np.float32)[:, None] * np.float32(THETA) ** (-np.arange(half, dtype=np.float32) / np.float32(half))
    cos, sin = np.cos(angle.astype(np.float64)), np.sin(angle.astype(np.float64))
    return np.stack([np.concatenate([cos, cos], -1), np.concatenate([-sin, sin], -1)]).astype(np.float32)


def solution(mesh):
    n = mesh.shape["tp"]

    def step(x, gain, wq, wk, wv, wo):
        rows, width = x.shape
        inner, kv_inner = wq.shape[1], wk.shape[1]
        heads, kv = inner // HEAD, kv_inner // HEAD
        half, tokens, span = rows // 2, n * rows, PIECES * TILE
        spans, depth = width // span, width // PIECES
        strips = kv * -(-(heads // kv) // 2)
        bf16, f32 = jnp.bfloat16, jnp.float32
        anywhere = pl.BlockSpec(memory_space=pl.ANY)
        return pl.pallas_call(
            functools.partial(_kernel, n, heads, kv),
            out_shape=pltpu.VMEM((rows, width), bf16),
            in_specs=[anywhere] * 7,
            out_specs=pl.BlockSpec(memory_space=pltpu.VMEM),
            scratch_shapes=[
                pltpu.VMEM((tokens, width), bf16),
                pltpu.VMEM((rows, width), bf16),
                pltpu.VMEM((heads + 2 * kv, tokens, HEAD), bf16),
                pltpu.VMEM((2, 2, spans, half, span), bf16),
                pltpu.VMEM((2, 3, spans, half, span), bf16),
                pltpu.VMEM((rows, span), f32),
                pltpu.VMEM((SLOTS, PIECES, depth, TILE), bf16),
                pltpu.VMEM((2, tokens, HEAD), f32),
                pltpu.VMEM((width // HEAD, HEAD), bf16),
                pltpu.VMEM((1, width), f32),
                pltpu.VMEM((strips, 2 * half), f32),
                pltpu.VMEM((strips, HEAD + 8, 2 * half), f32),
                pltpu.SemaphoreType.DMA((2, 3, 2)),
                pltpu.SemaphoreType.DMA((2, 3, 2)),
                pltpu.SemaphoreType.DMA((2, 3, spans)),
                pltpu.SemaphoreType.DMA((2, 3, spans)),
                pltpu.SemaphoreType.DMA((SLOTS,)),
                pltpu.SemaphoreType.DMA((3,)),
                pltpu.SemaphoreType.REGULAR,
            ],
            compiler_params=pltpu.CompilerParams(collective_id=0, has_side_effects=True, vmem_limit_bytes=VMEM),
        )(x, gain.reshape(width // HEAD, HEAD), _turns(tokens), wq.reshape(PIECES, depth, inner), wk.reshape(PIECES, depth, kv_inner),
          wv.reshape(PIECES, depth, kv_inner), wo)

    tokens, columns = P(("dp", "tp"), None), P(None, "tp")
    return jax.shard_map(
        step,
        mesh=mesh,
        in_specs=(tokens, P(None), columns, columns, columns, P("tp", None)),
        out_specs=tokens,
        check_vma=False,
    )
```

```python
import functools

import jax
import jax.numpy as jnp
import numpy as np
from jax import lax
from jax.experimental import pallas as pl
from jax.experimental.pallas import tpu as pltpu
from jax.sharding import PartitionSpec as P

HEAD = 128
THETA = 10000
NEG = -1e30
HIDDEN = 2 * NEG
LOG2E = 1.4426950408889634
VMEM = 63_000_000
MESH = pl.DeviceIdType.MESH

TILE = 256
PIECES = 4
SLOTS = 3
KEYS = 256
FIRST, PASSED, SECOND = 0, 1, 2
OWN, VIA, SUM = 0, 1, 2


def _dot(a, b, ca=1, cb=0):
    return lax.dot_general(a, b, (((ca,), (cb,)), ((), ())), preferred_element_type=jnp.float32)


def _kernel(n, heads, kv, x_ref, gain_ref, turn_ref, wq_ref, wk_ref, wv_ref, wo_ref, y_ref,
            xs, nb, qkv, sends, recvs, own, wbuf, turn, gain_in, gain, top_s, mix_s,
            ag_send, ag_recv, rs_send, rs_recv, wsem, lsem, here_sem):
    me = lax.axis_index("tp")
    right, left, far = lax.rem(me + 1, n), lax.rem(me + n - 1, n), lax.rem(me + 2, n)
    sides = ((right, left), (left, right))
    rows, width = x_ref.shape
    half, sub = rows // 2, rows // 4
    group = heads // kv
    inner = heads * HEAD
    depth = width // PIECES
    q_tiles = inner // TILE
    span = PIECES * TILE
    spans = width // span

    load_turn = pltpu.make_async_copy(turn_ref, turn, lsem.at[0])
    load_gain = pltpu.make_async_copy(gain_ref, gain_in, lsem.at[1])

    load_x = pltpu.make_async_copy(x_ref, xs.at[pl.ds(pl.multiple_of(me * rows, rows), rows)], lsem.at[2])


    def fetch_q(j, slot):
        @pl.when(j < q_tiles)
        def _():
            at = pl.ds(pl.multiple_of(j * TILE, TILE), TILE)
            pltpu.make_async_copy(wq_ref.at[:, :, at], wbuf.at[slot], wsem.at[slot]).start()

        @pl.when(j == q_tiles)
        def _():
            pltpu.make_async_copy(wk_ref, wbuf.at[slot], wsem.at[slot]).start()

        @pl.when(j == q_tiles + 1)
        def _():
            pltpu.make_async_copy(wv_ref, wbuf.at[slot], wsem.at[slot]).start()

    def fetch_o(j, slot):
        for c in range(PIECES):
            at = pl.ds(pl.multiple_of(j * span + c * TILE, TILE), TILE)
            pltpu.make_async_copy(wo_ref.at[:, at], wbuf.at[slot, c], wsem.at[slot]).start()

    passes = (fetch_q, fetch_q, fetch_q, fetch_o, fetch_q, fetch_o, fetch_o, fetch_o)
    lengths = [q_tiles + 2 if f is fetch_q else spans for f in passes]

    def stream(index, body):
        fetch, length, before = passes[index], lengths[index], sum(lengths[:index])

        @pl.loop(0, length)
        def _(j):
            slot = lax.rem(before + j, SLOTS)
            pltpu.make_async_copy(wk_ref, wbuf.at[slot], wsem.at[slot]).wait()
            body(j, slot)

            @pl.when(j + SLOTS < length)
            def _():
                fetch(j + SLOTS, slot)

            if index + 1 < len(passes):
                @pl.when(j + SLOTS >= length)
                def _():
                    passes[index + 1](j + SLOTS - length, slot)

    def gathered(way, kind):
        source = sides[way][1]
        near = source * rows + way * half
        return pl.multiple_of(jnp.where(kind == PASSED, far * rows + way * half,
                                        jnp.where(kind == SECOND, source * rows + (1 - way) * half, near)), half)

    def arrival(way, kind, s):
        here = xs.at[pl.ds(pl.multiple_of(gathered(way, kind) + s * sub, sub), sub)]
        return pltpu.make_async_remote_copy(here, here, ag_send.at[way, kind, s], ag_recv.at[way, kind, s],
                                            device_id={"tp": sides[way][1]}, device_id_type=MESH)

    def gather(way, kind, s):
        if kind == PASSED:
            at = gathered(way, FIRST) + s * sub
            source = xs.at[pl.ds(pl.multiple_of(at, sub), sub)]
        else:
            place = (way if kind == FIRST else 1 - way) * half + s * sub
            at = me * rows + place
            source = x_ref.at[pl.ds(place, sub)]
        return pltpu.make_async_remote_copy(source, xs.at[pl.ds(pl.multiple_of(at, sub), sub)], ag_send.at[way, kind, s], ag_recv.at[way, kind, s],
                                            device_id={"tp": sides[way][0]}, device_id_type=MESH)

    def scatter(way, kind, buffer, turn_no, j):
        return pltpu.make_async_remote_copy(sends.at[way, buffer, j], recvs.at[way, kind, j], rs_send.at[way, turn_no, j],
                                            rs_recv.at[way, kind, j], device_id={"tp": sides[way][0]}, device_id_type=MESH)

    def project(index, places):
        for p, place in enumerate(places):
            @pl.loop(0, half // 16)
            def _(i):
                here = pl.ds(pl.multiple_of(place + i * 16, 16), 16)
                there = pl.ds(pl.multiple_of(p * half + i * 16, 16), 16)
                squares = jnp.zeros((16, span), jnp.float32)
                for c in range(spans):
                    wide = xs[here, c * span : (c + 1) * span].astype(jnp.float32)
                    squares += wide * wide
                scale = lax.rsqrt(jnp.sum(squares, -1, keepdims=True) * (1 / width) + 1e-6)
                for c in range(spans):
                    wide = xs[here, c * span : (c + 1) * span].astype(jnp.float32)
                    nb[there, c * span : (c + 1) * span] = (wide * scale * gain[:, c * span : (c + 1) * span]).astype(jnp.bfloat16)

        def body(j, slot):
            t = _dot(nb[:, :depth], wbuf[slot, 0])
            for c in range(1, PIECES):
                t += _dot(nb[:, c * depth : (c + 1) * depth], wbuf[slot, c])
            t = t.astype(jnp.bfloat16)
            for p, place in enumerate(places):
                here = pl.ds(place, half)
                for h in range(TILE // HEAD):
                    head = t[p * half : (p + 1) * half, h * HEAD : (h + 1) * HEAD]

                    @pl.when(j <= q_tiles)
                    def _():
                        wide = head.astype(jnp.float32)
                        turned = wide * turn[0, here, :] + pltpu.roll(wide, HEAD // 2, 1) * turn[1, here, :]
                        qkv[j * (TILE // HEAD) + h, here, :] = turned.astype(jnp.bfloat16)

                    @pl.when(j > q_tiles)
                    def _():
                        qkv[j * (TILE // HEAD) + h, here, :] = head

        stream(index, body)

    strips = [(g, list(range(g * group + i, min(g * group + i + 2, (g + 1) * group)))) for g in range(kv) for i in range(0, group, 2)]

    def attend(places):
        e = HEAD**-0.5 * LOG2E
        ones = jnp.ones((8, KEYS), jnp.bfloat16)

        @pl.loop(0, len(places))
        def _(unit):
            place = pl.multiple_of(jnp.where(unit == 0, places[0], places[1]), half)
            mine = pl.ds(place, half)
            top_s[...] = jnp.full(top_s.shape, NEG, jnp.float32)
            mix_s[...] = jnp.zeros(mix_s.shape, jnp.float32)

            def block(j, masked):
                here = pl.ds(pl.multiple_of(j * KEYS, KEYS), KEYS)
                scores, weights, keeps = [], [], []
                for g, hs in strips:
                    q = jnp.concatenate([qkv[h, mine, :] for h in hs], axis=0)
                    scores.append(_dot(qkv[heads + g, here, :], q, 1, 1))
                if masked:
                    shape = (KEYS, 2 * half)
                    gap = lax.rem(lax.broadcasted_iota(jnp.int32, shape, 1), half) - lax.broadcasted_iota(jnp.int32, shape, 0)
                    ok = gap >= j * KEYS - place
                for i, s in enumerate(scores):
                    wide = s.shape[1]
                    if masked:
                        s = jnp.where(ok[:, :wide], s, HIDDEN)
                    old = top_s[i : i + 1, :wide]
                    top = jnp.maximum(old, s.max(axis=0, keepdims=True))
                    top_s[i : i + 1, :wide] = top
                    weights.append(jnp.exp2((s - top) * e).astype(jnp.bfloat16))
                    keeps.append(jnp.exp2((old - top) * e))
                for i, (g, hs) in enumerate(strips):
                    wide = len(hs) * half
                    values = jnp.concatenate([qkv[heads + kv + g, here, :].T, ones], axis=0)
                    mix_s[i, :, :wide] = mix_s[i, :, :wide] * keeps[i] + _dot(values, weights[i])

            whole = lax.div(place, KEYS)

            @pl.loop(0, whole)
            def _(j):
                block(j, False)

            block(whole, True)
            for i, (g, hs) in enumerate(strips):
                wide = len(hs) * half
                out = (mix_s[i, :HEAD, :wide] * (1 / mix_s[i, HEAD : HEAD + 1, :wide])).T.astype(jnp.bfloat16)
                for m, h in enumerate(hs):
                    qkv[h, mine, :] = out[m * half : (m + 1) * half, :]

    def terms(index, places, before, emit):
        for p, place in enumerate(places):
            for h in range(heads):
                nb[p * half : (p + 1) * half, h * HEAD : (h + 1) * HEAD] = qkv[h, pl.ds(place, half), :]

        def body(j, slot):
            before(j)
            for c in range(PIECES):
                emit(j, slice(c * TILE, (c + 1) * TILE), _dot(nb[:, :inner], wbuf[slot, c]))

        stream(index, body)

    def send_terms(index, places, kinds, turn_no):
        buffer = turn_no % 2

        def before(j):
            @pl.when(j > 0)
            def _():
                for way in range(2):
                    scatter(way, kinds[way], buffer, turn_no, j - 1).start()

            if turn_no == 2:
                for way in range(2):
                    scatter(way, OWN, buffer, 0, j).wait_send()
                    scatter(way, VIA, buffer, turn_no, j).wait_recv()

        def emit(j, columns, t):
            for way in range(2):
                mine = t[way * half : (way + 1) * half]
                if turn_no == 2:
                    mine += recvs[way, VIA, j, :, columns].astype(jnp.float32)
                sends[way, buffer, j, :, columns] = mine.astype(jnp.bfloat16)

        terms(index, places, before, emit)
        for way in range(2):
            scatter(way, kinds[way], buffer, turn_no, spans - 1).start()

    barrier = pltpu.get_barrier_semaphore()
    pl.semaphore_signal(barrier, inc=1, device_id={"tp": left}, device_id_type=MESH)
    pl.semaphore_wait(barrier, 1)
    pl.semaphore_signal(here_sem, inc=1, device_id={"tp": right}, device_id_type=MESH)
    pass_first = (me > 0, me == n - 1)
    for way in range(2):
        if way == 1:
            pl.semaphore_wait(here_sem, 1)
        for s in range(2):
            gather(way, FIRST, s).start()
    load_x.start()
    load_gain.start()
    for j in range(SLOTS):
        passes[0](jnp.int32(j), j)
    load_turn.start()
    for s in range(2):
        for way in range(2):
            @pl.when(jnp.logical_not(pass_first[way]))
            def _():
                gather(way, SECOND, s).start()

    qkv[heads:] = jnp.zeros((2 * kv, *qkv.shape[1:]), jnp.bfloat16)
    load_x.wait()
    load_gain.wait()
    load_turn.wait()
    wide_gain = gain_in[...].astype(jnp.float32)
    for i in range(width // HEAD):
        gain[:, i * HEAD : (i + 1) * HEAD] = wide_gain[i : i + 1, :]
    project(0, (pl.multiple_of(me * rows, rows), pl.multiple_of(me * rows + half, half)))
    for s in range(2):
        for way in range(2):
            arrival(way, FIRST, s).wait_recv()
            gather(way, PASSED, s).start()
    for s in range(2):
        for way in range(2):
            @pl.when(pass_first[way])
            def _():
                gather(way, SECOND, s).start()
    project(1, (gathered(0, FIRST), gathered(1, FIRST)))

    second = (jnp.where(left > 0, PASSED, SECOND), jnp.where(right == n - 1, PASSED, SECOND))
    third = tuple(PASSED + SECOND - kind for kind in second)
    for index, kinds in ((2, second), (4, third)):
        for s in range(2):
            for way in range(2):
                arrival(way, kinds[way], s).wait_recv()
        project(index, (gathered(0, kinds[0]), gathered(1, kinds[1])))

        def scattered(way, kind):
            to = sides[way][0]
            return pl.multiple_of(jnp.where(kind == VIA, far * rows + (1 - way) * half,
                                            jnp.where(kind == OWN, to * rows + way * half, to * rows + (1 - way) * half)), half)

        early = tuple(jnp.where(sides[way][0] < far, OWN, VIA) for way in range(2))
        late = tuple(OWN + VIA - kind for kind in early)
        kinds = early if index == 2 else late
        places = tuple(scattered(way, kinds[way]) for way in range(2))
        attend(places)
        send_terms(index + 1, places, kinds, 0 if index == 2 else 1)

    kinds = (SUM, SUM)
    places = tuple(scattered(way, SUM) for way in range(2))
    attend(places)
    send_terms(6, places, kinds, 2)

    places = (pl.multiple_of(me * rows, rows), pl.multiple_of(me * rows + half, half))
    attend(places)

    def finish(j, columns, t):
        own[:, columns] = t
        if columns.stop < span:
            return
        at = pl.ds(pl.multiple_of(j * span, span), span)
        halves = (slice(0, half), slice(half, rows))
        for p in range(2):
            scatter(p, OWN, 0, 2, j).wait_recv()
            x_part = xs[pl.ds(pl.multiple_of(places[p], half), half), at].astype(jnp.float32)
            own[halves[p], :] = own[halves[p], :] + x_part + recvs[p, OWN, j].astype(jnp.float32)

        @pl.when(j > 0)
        def _():
            for way in range(2):
                scatter(way, SUM, 0, 2, j - 1).wait_send()

        for p in (1, 0):
            scatter(1 - p, SUM, 0, 2, j).wait_recv()
            y_ref[halves[p], at] = (own[halves[p], :] + recvs[1 - p, SUM, j].astype(jnp.float32)).astype(jnp.bfloat16)

    for way in range(2):
        for kind in (FIRST, PASSED, SECOND):
            for s in range(2):
                gather(way, kind, s).wait_send()

    @pl.loop(0, spans)
    def _(j):
        for way in range(2):
            scatter(way, late[way], 1, 1, j).wait_send()

    terms(7, places, lambda j: None, finish)
    for way in range(2):
        scatter(way, SUM, 0, 2, spans - 1).wait_send()


def _put(parts, y_ref, out_ref, sem):
    rows = y_ref.shape[0] // parts
    copies = [pltpu.make_async_copy(y_ref.at[pl.ds(i * rows, rows)], out_ref.at[pl.ds(i * rows, rows)], sem.at[i]) for i in range(parts)]
    for copy in copies:
        copy.start()
    for copy in copies:
        copy.wait()


def _turns(tokens):
    half = HEAD // 2
    angle = np.arange(tokens, dtype=np.float32)[:, None] * np.float32(THETA) ** (-np.arange(half, dtype=np.float32) / np.float32(half))
    cos, sin = np.cos(angle.astype(np.float64)), np.sin(angle.astype(np.float64))
    return np.stack([np.concatenate([cos, cos], -1), np.concatenate([-sin, sin], -1)]).astype(np.float32)


def solution(mesh):
    n = mesh.shape["tp"]

    def step(x, gain, wq, wk, wv, wo):
        rows, width = x.shape
        inner, kv_inner = wq.shape[1], wk.shape[1]
        heads, kv = inner // HEAD, kv_inner // HEAD
        half, tokens, span = rows // 2, n * rows, PIECES * TILE
        spans, depth = width // span, width // PIECES
        strips = kv * -(-(heads // kv) // 2)
        bf16, f32 = jnp.bfloat16, jnp.float32
        anywhere = pl.BlockSpec(memory_space=pl.ANY)
        y = pl.pallas_call(
            functools.partial(_kernel, n, heads, kv),
            out_shape=pltpu.VMEM((rows, width), bf16),
            in_specs=[anywhere] * 7,
            out_specs=pl.BlockSpec(memory_space=pltpu.VMEM),
            scratch_shapes=[
                pltpu.VMEM((tokens, width), bf16),
                pltpu.VMEM((rows, width), bf16),
                pltpu.VMEM((heads + 2 * kv, tokens, HEAD), bf16),
                pltpu.VMEM((2, 2, spans, half, span), bf16),
                pltpu.VMEM((2, 3, spans, half, span), bf16),
                pltpu.VMEM((rows, span), f32),
                pltpu.VMEM((SLOTS, PIECES, depth, TILE), bf16),
                pltpu.VMEM((2, tokens, HEAD), f32),
                pltpu.VMEM((width // HEAD, HEAD), bf16),
                pltpu.VMEM((1, width), f32),
                pltpu.VMEM((strips, 2 * half), f32),
                pltpu.VMEM((strips, HEAD + 8, 2 * half), f32),
                pltpu.SemaphoreType.DMA((2, 3, 2)),
                pltpu.SemaphoreType.DMA((2, 3, 2)),
                pltpu.SemaphoreType.DMA((2, 3, spans)),
                pltpu.SemaphoreType.DMA((2, 3, spans)),
                pltpu.SemaphoreType.DMA((SLOTS,)),
                pltpu.SemaphoreType.DMA((3,)),
                pltpu.SemaphoreType.REGULAR,
            ],
            compiler_params=pltpu.CompilerParams(collective_id=0, has_side_effects=True, vmem_limit_bytes=VMEM),
        )(x, gain.reshape(width // HEAD, HEAD), _turns(tokens), wq.reshape(PIECES, depth, inner), wk.reshape(PIECES, depth, kv_inner),
          wv.reshape(PIECES, depth, kv_inner), wo)
        return pl.pallas_call(
            functools.partial(_put, 4),
            out_shape=jax.ShapeDtypeStruct((rows, width), bf16),
            in_specs=[pl.BlockSpec(memory_space=pltpu.VMEM)],
            out_specs=anywhere,
            scratch_shapes=[pltpu.SemaphoreType.DMA((4,))],
            compiler_params=pltpu.CompilerParams(vmem_limit_bytes=2**20),
        )(pltpu.with_memory_space_constraint(y, pltpu.VMEM))

    tokens, columns = P(("dp", "tp"), None), P(None, "tp")
    return jax.shard_map(
        step,
        mesh=mesh,
        in_specs=(tokens, P(None), columns, columns, columns, P("tp", None)),
        out_specs=tokens,
        check_vma=False,
    )
```

```python
import functools

import jax
import jax.numpy as jnp
import numpy as np
from jax import lax
from jax.experimental import pallas as pl
from jax.experimental.pallas import tpu as pltpu
from jax.sharding import PartitionSpec as P

HEAD = 128
THETA = 10000
HIDDEN = float("-inf")
LOG2E = 1.4426950408889634
VMEM = 63_000_000
MESH = pl.DeviceIdType.MESH

TILE = 256
PIECES = 4
SLOTS = 3
KEYS = 256
FIRST, PASSED, SECOND = 0, 1, 2
OWN, VIA, SUM = 0, 1, 2


def _dot(a, b, ca=1, cb=0):
    return lax.dot_general(a, b, (((ca,), (cb,)), ((), ())), preferred_element_type=jnp.float32)


def _kernel(n, heads, kv, x_ref, gain_ref, turn_ref, wq_ref, wk_ref, wv_ref, wo_ref, y_ref,
            xs, nb, qkv, sends, recvs, own, wbuf, turn, gain_in, gain, top_s, mix_s,
            ag_send, ag_recv, rs_send, rs_recv, wsem, lsem, here_sem):
    me = lax.axis_index("tp")
    right, left, far = lax.rem(me + 1, n), lax.rem(me + n - 1, n), lax.rem(me + 2, n)
    sides = ((right, left), (left, right))
    rows, width = x_ref.shape
    half, sub = rows // 2, rows // 4
    group = heads // kv
    inner = heads * HEAD
    depth = width // PIECES
    q_tiles = inner // TILE
    span = PIECES * TILE
    spans = width // span

    load_turn = pltpu.make_async_copy(turn_ref, turn, lsem.at[0])
    load_gain = pltpu.make_async_copy(gain_ref, gain_in, lsem.at[1])

    load_x = pltpu.make_async_copy(x_ref, xs.at[pl.ds(pl.multiple_of(me * rows, rows), rows)], lsem.at[2])


    def fetch_q(j, slot):
        @pl.when(j < q_tiles)
        def _():
            at = pl.ds(pl.multiple_of(j * TILE, TILE), TILE)
            pltpu.make_async_copy(wq_ref.at[:, :, at], wbuf.at[slot], wsem.at[slot]).start()

        @pl.when(j == q_tiles)
        def _():
            pltpu.make_async_copy(wk_ref, wbuf.at[slot], wsem.at[slot]).start()

        @pl.when(j == q_tiles + 1)
        def _():
            pltpu.make_async_copy(wv_ref, wbuf.at[slot], wsem.at[slot]).start()

    def fetch_o(j, slot):
        for c in range(PIECES):
            at = pl.ds(pl.multiple_of(j * span + c * TILE, TILE), TILE)
            pltpu.make_async_copy(wo_ref.at[:, at], wbuf.at[slot, c], wsem.at[slot]).start()

    passes = (fetch_q, fetch_q, fetch_q, fetch_o, fetch_q, fetch_o, fetch_o, fetch_o)
    lengths = [q_tiles + 2 if f is fetch_q else spans for f in passes]

    def stream(index, body):
        fetch, length, before = passes[index], lengths[index], sum(lengths[:index])

        @pl.loop(0, length)
        def _(j):
            slot = lax.rem(before + j, SLOTS)
            pltpu.make_async_copy(wk_ref, wbuf.at[slot], wsem.at[slot]).wait()
            body(j, slot)

            @pl.when(j + SLOTS < length)
            def _():
                fetch(j + SLOTS, slot)

            if index + 1 < len(passes):
                @pl.when(j + SLOTS >= length)
                def _():
                    passes[index + 1](j + SLOTS - length, slot)

    def gathered(way, kind):
        source = sides[way][1]
        near = source * rows + way * half
        return pl.multiple_of(jnp.where(kind == PASSED, far * rows + way * half,
                                        jnp.where(kind == SECOND, source * rows + (1 - way) * half, near)), half)

    def arrival(way, kind, s):
        here = xs.at[pl.ds(pl.multiple_of(gathered(way, kind) + s * sub, sub), sub)]
        return pltpu.make_async_remote_copy(here, here, ag_send.at[way, kind, s], ag_recv.at[way, kind, s],
                                            device_id={"tp": sides[way][1]}, device_id_type=MESH)

    def gather(way, kind, s):
        if kind == PASSED:
            at = gathered(way, FIRST) + s * sub
            source = xs.at[pl.ds(pl.multiple_of(at, sub), sub)]
        else:
            place = (way if kind == FIRST else 1 - way) * half + s * sub
            at = me * rows + place
            source = x_ref.at[pl.ds(place, sub)]
        return pltpu.make_async_remote_copy(source, xs.at[pl.ds(pl.multiple_of(at, sub), sub)], ag_send.at[way, kind, s], ag_recv.at[way, kind, s],
                                            device_id={"tp": sides[way][0]}, device_id_type=MESH)

    def scatter(way, kind, buffer, turn_no, j):
        return pltpu.make_async_remote_copy(sends.at[way, buffer, j], recvs.at[way, kind, j], rs_send.at[way, turn_no, j],
                                            rs_recv.at[way, kind, j], device_id={"tp": sides[way][0]}, device_id_type=MESH)

    def project(index, places):
        for p, place in enumerate(places):
            @pl.loop(0, half // 16)
            def _(i):
                here = pl.ds(pl.multiple_of(place + i * 16, 16), 16)
                there = pl.ds(pl.multiple_of(p * half + i * 16, 16), 16)
                squares = jnp.zeros((16, span), jnp.float32)
                for c in range(spans):
                    wide = xs[here, c * span : (c + 1) * span].astype(jnp.float32)
                    squares += wide * wide
                scale = lax.rsqrt(jnp.sum(squares, -1, keepdims=True) * (1 / width) + 1e-6)
                for c in range(spans):
                    wide = xs[here, c * span : (c + 1) * span].astype(jnp.float32)
                    nb[there, c * span : (c + 1) * span] = (wide * scale * gain[:, c * span : (c + 1) * span]).astype(jnp.bfloat16)

        def body(j, slot):
            t = _dot(nb[:, :depth], wbuf[slot, 0])
            for c in range(1, PIECES):
                t += _dot(nb[:, c * depth : (c + 1) * depth], wbuf[slot, c])
            t = t.astype(jnp.bfloat16)
            for p, place in enumerate(places):
                here = pl.ds(place, half)
                for h in range(TILE // HEAD):
                    head = t[p * half : (p + 1) * half, h * HEAD : (h + 1) * HEAD]

                    @pl.when(j <= q_tiles)
                    def _():
                        wide = head.astype(jnp.float32)
                        turned = wide * turn[0, here, :] + pltpu.roll(wide, HEAD // 2, 1) * turn[1, here, :]
                        qkv[j * (TILE // HEAD) + h, here, :] = turned.astype(jnp.bfloat16)

                    @pl.when(j > q_tiles)
                    def _():
                        qkv[j * (TILE // HEAD) + h, here, :] = head

        stream(index, body)

    strips = [(g, list(range(g * group + i, min(g * group + i + 2, (g + 1) * group)))) for g in range(kv) for i in range(0, group, 2)]

    def attend(places):
        e = HEAD**-0.5 * LOG2E
        ones = jnp.ones((8, KEYS), jnp.bfloat16)

        @pl.loop(0, len(places))
        def _(unit):
            place = pl.multiple_of(jnp.where(unit == 0, places[0], places[1]), half)
            mine = pl.ds(place, half)
            top_s[...] = jnp.full(top_s.shape, HIDDEN, jnp.float32)
            mix_s[...] = jnp.zeros(mix_s.shape, jnp.float32)

            def block(j, masked):
                here = pl.ds(pl.multiple_of(j * KEYS, KEYS), KEYS)
                scores, weights, keeps = [], [], []
                for g, hs in strips:
                    q = jnp.concatenate([qkv[h, mine, :] for h in hs], axis=0)
                    scores.append(_dot(qkv[heads + g, here, :], q, 1, 1))
                if masked:
                    shape = (KEYS, 2 * half)
                    gap = lax.rem(lax.broadcasted_iota(jnp.int32, shape, 1), half) - lax.broadcasted_iota(jnp.int32, shape, 0)
                    ok = gap >= j * KEYS - place
                for i, s in enumerate(scores):
                    wide = s.shape[1]
                    if masked:
                        s = jnp.where(ok[:, :wide], s, HIDDEN)
                    old = top_s[i : i + 1, :wide]
                    top = jnp.maximum(old, s.max(axis=0, keepdims=True))
                    top_s[i : i + 1, :wide] = top
                    weights.append(jnp.exp2((s - top) * e).astype(jnp.bfloat16))
                    keeps.append(jnp.exp2((old - top) * e))
                for i, (g, hs) in enumerate(strips):
                    wide = len(hs) * half
                    values = jnp.concatenate([qkv[heads + kv + g, here, :].T, ones], axis=0)
                    mix_s[i, :, :wide] = mix_s[i, :, :wide] * keeps[i] + _dot(values, weights[i])

            whole = lax.div(place, KEYS)

            @pl.loop(0, whole)
            def _(j):
                block(j, False)

            block(whole, True)
            for i, (g, hs) in enumerate(strips):
                wide = len(hs) * half
                out = (mix_s[i, :HEAD, :wide] * (1 / mix_s[i, HEAD : HEAD + 1, :wide])).T.astype(jnp.bfloat16)
                for m, h in enumerate(hs):
                    qkv[h, mine, :] = out[m * half : (m + 1) * half, :]

    def terms(index, places, before, emit, during=None):
        for p, place in enumerate(places):
            for h in range(heads):
                nb[p * half : (p + 1) * half, h * HEAD : (h + 1) * HEAD] = qkv[h, pl.ds(place, half), :]

        def body(j, slot):
            before(j)
            for c in range(PIECES):
                emit(j, slice(c * TILE, (c + 1) * TILE), _dot(nb[:, :inner], wbuf[slot, c]))
                if during is not None and c == 0:
                    during(j)

        stream(index, body)

    def send_terms(index, places, kinds, turn_no):
        buffer = turn_no % 2

        def during(j):
            @pl.when(j > 0)
            def _():
                for way in range(2):
                    scatter(way, kinds[way], buffer, turn_no, j - 1).start()

        def before(j):
            if turn_no == 2:
                for way in range(2):
                    scatter(way, OWN, buffer, 0, j).wait_send()
                    scatter(way, VIA, buffer, turn_no, j).wait_recv()

        def emit(j, columns, t):
            for way in range(2):
                mine = t[way * half : (way + 1) * half]
                if turn_no == 2:
                    mine += recvs[way, VIA, j, :, columns].astype(jnp.float32)
                sends[way, buffer, j, :, columns] = mine.astype(jnp.bfloat16)

        terms(index, places, before, emit, during)
        for way in range(2):
            scatter(way, kinds[way], buffer, turn_no, spans - 1).start()

    barrier = pltpu.get_barrier_semaphore()
    pl.semaphore_signal(barrier, inc=1, device_id={"tp": left}, device_id_type=MESH)
    pl.semaphore_wait(barrier, 1)
    pl.semaphore_signal(here_sem, inc=1, device_id={"tp": right}, device_id_type=MESH)
    pass_first = (me > 0, me == n - 1)
    for way in range(2):
        if way == 1:
            pl.semaphore_wait(here_sem, 1)
        for s in range(2):
            gather(way, FIRST, s).start()
    load_x.start()
    load_gain.start()
    for j in range(SLOTS):
        passes[0](jnp.int32(j), j)
    load_turn.start()
    for s in range(2):
        for way in range(2):
            @pl.when(jnp.logical_not(pass_first[way]))
            def _():
                gather(way, SECOND, s).start()

    qkv[heads:] = jnp.zeros((2 * kv, *qkv.shape[1:]), jnp.bfloat16)
    load_x.wait()
    load_gain.wait()
    load_turn.wait()
    wide_gain = gain_in[...].astype(jnp.float32)
    for i in range(width // HEAD):
        gain[:, i * HEAD : (i + 1) * HEAD] = wide_gain[i : i + 1, :]
    project(0, (pl.multiple_of(me * rows, rows), pl.multiple_of(me * rows + half, half)))
    for s in range(2):
        for way in range(2):
            arrival(way, FIRST, s).wait_recv()
            gather(way, PASSED, s).start()
    for s in range(2):
        for way in range(2):
            @pl.when(pass_first[way])
            def _():
                gather(way, SECOND, s).start()
    project(1, (gathered(0, FIRST), gathered(1, FIRST)))

    second = (jnp.where(left > 0, PASSED, SECOND), jnp.where(right == n - 1, PASSED, SECOND))
    third = tuple(PASSED + SECOND - kind for kind in second)
    for index, kinds in ((2, second), (4, third)):
        for s in range(2):
            for way in range(2):
                arrival(way, kinds[way], s).wait_recv()
        project(index, (gathered(0, kinds[0]), gathered(1, kinds[1])))

        def scattered(way, kind):
            to = sides[way][0]
            return pl.multiple_of(jnp.where(kind == VIA, far * rows + (1 - way) * half,
                                            jnp.where(kind == OWN, to * rows + way * half, to * rows + (1 - way) * half)), half)

        early = tuple(jnp.where(sides[way][0] < far, OWN, VIA) for way in range(2))
        late = tuple(OWN + VIA - kind for kind in early)
        kinds = early if index == 2 else late
        places = tuple(scattered(way, kinds[way]) for way in range(2))
        attend(places)
        send_terms(index + 1, places, kinds, 0 if index == 2 else 1)

    kinds = (SUM, SUM)
    places = tuple(scattered(way, SUM) for way in range(2))
    attend(places)
    send_terms(6, places, kinds, 2)

    places = (pl.multiple_of(me * rows, rows), pl.multiple_of(me * rows + half, half))
    attend(places)

    def finish(j, columns, t):
        own[:, columns] = t
        if columns.stop < span:
            return
        at = pl.ds(pl.multiple_of(j * span, span), span)
        halves = (slice(0, half), slice(half, rows))
        for p in range(2):
            scatter(p, OWN, 0, 2, j).wait_recv()
            x_part = xs[pl.ds(pl.multiple_of(places[p], half), half), at].astype(jnp.float32)
            own[halves[p], :] = own[halves[p], :] + x_part + recvs[p, OWN, j].astype(jnp.float32)

        @pl.when(j > 0)
        def _():
            for way in range(2):
                scatter(way, SUM, 0, 2, j - 1).wait_send()

        for p in (1, 0):
            scatter(1 - p, SUM, 0, 2, j).wait_recv()
            y_ref[halves[p], at] = (own[halves[p], :] + recvs[1 - p, SUM, j].astype(jnp.float32)).astype(jnp.bfloat16)

    for way in range(2):
        for kind in (FIRST, PASSED, SECOND):
            for s in range(2):
                gather(way, kind, s).wait_send()

    @pl.loop(0, spans)
    def _(j):
        for way in range(2):
            scatter(way, late[way], 1, 1, j).wait_send()

    terms(7, places, lambda j: None, finish)
    for way in range(2):
        scatter(way, SUM, 0, 2, spans - 1).wait_send()


def _turns(tokens):
    half = HEAD // 2
    angle = np.arange(tokens, dtype=np.float32)[:, None] * np.float32(THETA) ** (-np.arange(half, dtype=np.float32) / np.float32(half))
    cos, sin = np.cos(angle.astype(np.float64)), np.sin(angle.astype(np.float64))
    return np.stack([np.concatenate([cos, cos], -1), np.concatenate([-sin, sin], -1)]).astype(np.float32)


def solution(mesh):
    n = mesh.shape["tp"]

    def step(x, gain, wq, wk, wv, wo):
        rows, width = x.shape
        inner, kv_inner = wq.shape[1], wk.shape[1]
        heads, kv = inner // HEAD, kv_inner // HEAD
        half, tokens, span = rows // 2, n * rows, PIECES * TILE
        spans, depth = width // span, width // PIECES
        strips = kv * -(-(heads // kv) // 2)
        bf16, f32 = jnp.bfloat16, jnp.float32
        anywhere = pl.BlockSpec(memory_space=pl.ANY)
        return pl.pallas_call(
            functools.partial(_kernel, n, heads, kv),
            out_shape=pltpu.VMEM((rows, width), bf16),
            in_specs=[anywhere] * 7,
            out_specs=pl.BlockSpec(memory_space=pltpu.VMEM),
            scratch_shapes=[
                pltpu.VMEM((tokens, width), bf16),
                pltpu.VMEM((rows, width), bf16),
                pltpu.VMEM((heads + 2 * kv, tokens, HEAD), bf16),
                pltpu.VMEM((2, 2, spans, half, span), bf16),
                pltpu.VMEM((2, 3, spans, half, span), bf16),
                pltpu.VMEM((rows, span), f32),
                pltpu.VMEM((SLOTS, PIECES, depth, TILE), bf16),
                pltpu.VMEM((2, tokens, HEAD), f32),
                pltpu.VMEM((width // HEAD, HEAD), bf16),
                pltpu.VMEM((1, width), f32),
                pltpu.VMEM((strips, 2 * half), f32),
                pltpu.VMEM((strips, HEAD + 8, 2 * half), f32),
                pltpu.SemaphoreType.DMA((2, 3, 2)),
                pltpu.SemaphoreType.DMA((2, 3, 2)),
                pltpu.SemaphoreType.DMA((2, 3, spans)),
                pltpu.SemaphoreType.DMA((2, 3, spans)),
                pltpu.SemaphoreType.DMA((SLOTS,)),
                pltpu.SemaphoreType.DMA((3,)),
                pltpu.SemaphoreType.REGULAR,
            ],
            compiler_params=pltpu.CompilerParams(collective_id=0, has_side_effects=True, vmem_limit_bytes=VMEM),
        )(x, gain.reshape(width // HEAD, HEAD), _turns(tokens), wq.reshape(PIECES, depth, inner), wk.reshape(PIECES, depth, kv_inner),
          wv.reshape(PIECES, depth, kv_inner), wo)

    tokens, columns = P(("dp", "tp"), None), P(None, "tp")
    return jax.shard_map(
        step,
        mesh=mesh,
        in_specs=(tokens, P(None), columns, columns, columns, P("tp", None)),
        out_specs=tokens,
        check_vma=False,
    )
```

```python
import functools

import jax
import jax.numpy as jnp
import numpy as np
from jax import lax
from jax.experimental import pallas as pl
from jax.experimental.pallas import tpu as pltpu
from jax.sharding import PartitionSpec as P

HEAD = 128
THETA = 10000
HIDDEN = float("-inf")
LOG2E = 1.4426950408889634
VMEM = 63_000_000
MESH = pl.DeviceIdType.MESH

TILE = 256
PIECES = 4
SLOTS = 3
KEYS = 256
FIRST, PASSED, SECOND = 0, 1, 2
OWN, VIA, SUM = 0, 1, 2


def _dot(a, b, ca=1, cb=0):
    return lax.dot_general(a, b, (((ca,), (cb,)), ((), ())), preferred_element_type=jnp.float32)


def _kernel(n, heads, kv, x_ref, gain_ref, turn_ref, wq_ref, wk_ref, wv_ref, wo_ref, y_ref,
            xs, nb, qkv, sends, recvs, own, wbuf, turn, gain_in, gain, top_s, mix_s,
            ag_send, ag_recv, rs_send, rs_recv, wsem, lsem, here_sem):
    me = lax.axis_index("tp")
    right, left, far = lax.rem(me + 1, n), lax.rem(me + n - 1, n), lax.rem(me + 2, n)
    sides = ((right, left), (left, right))
    rows, width = x_ref.shape
    half, sub = rows // 2, rows // 4
    group = heads // kv
    inner = heads * HEAD
    depth = width // PIECES
    q_tiles = inner // TILE
    span = PIECES * TILE
    spans = width // span

    load_turn = pltpu.make_async_copy(turn_ref, turn, lsem.at[0])
    load_gain = pltpu.make_async_copy(gain_ref, gain_in, lsem.at[1])

    load_x = pltpu.make_async_copy(x_ref, xs.at[pl.ds(pl.multiple_of(me * rows, rows), rows)], lsem.at[2])


    def fetch_q(j, slot):
        @pl.when(j < q_tiles)
        def _():
            at = pl.ds(pl.multiple_of(j * TILE, TILE), TILE)
            pltpu.make_async_copy(wq_ref.at[:, :, at], wbuf.at[slot], wsem.at[slot]).start()

        @pl.when(j == q_tiles)
        def _():
            pltpu.make_async_copy(wk_ref, wbuf.at[slot], wsem.at[slot]).start()

        @pl.when(j == q_tiles + 1)
        def _():
            pltpu.make_async_copy(wv_ref, wbuf.at[slot], wsem.at[slot]).start()

    def fetch_o(j, slot):
        for c in range(PIECES):
            at = pl.ds(pl.multiple_of(j * span + c * TILE, TILE), TILE)
            pltpu.make_async_copy(wo_ref.at[:, at], wbuf.at[slot, c], wsem.at[slot]).start()

    passes = (fetch_q, fetch_q, fetch_q, fetch_o, fetch_q, fetch_o, fetch_o, fetch_o)
    lengths = [q_tiles + 2 if f is fetch_q else spans for f in passes]

    def stream(index, body):
        fetch, length, before = passes[index], lengths[index], sum(lengths[:index])

        @pl.loop(0, length)
        def _(j):
            slot = lax.rem(before + j, SLOTS)
            pltpu.make_async_copy(wk_ref, wbuf.at[slot], wsem.at[slot]).wait()
            body(j, slot)

            @pl.when(j + SLOTS < length)
            def _():
                fetch(j + SLOTS, slot)

            if index + 1 < len(passes):
                @pl.when(j + SLOTS >= length)
                def _():
                    passes[index + 1](j + SLOTS - length, slot)

    def gathered(way, kind):
        source = sides[way][1]
        near = source * rows + way * half
        return pl.multiple_of(jnp.where(kind == PASSED, far * rows + way * half,
                                        jnp.where(kind == SECOND, source * rows + (1 - way) * half, near)), half)

    def arrival(way, kind, s):
        here = xs.at[pl.ds(pl.multiple_of(gathered(way, kind) + s * sub, sub), sub)]
        return pltpu.make_async_remote_copy(here, here, ag_send.at[way, kind, s], ag_recv.at[way, kind, s],
                                            device_id={"tp": sides[way][1]}, device_id_type=MESH)

    def gather(way, kind, s):
        if kind == PASSED:
            at = gathered(way, FIRST) + s * sub
            source = xs.at[pl.ds(pl.multiple_of(at, sub), sub)]
        else:
            place = (way if kind == FIRST else 1 - way) * half + s * sub
            at = me * rows + place
            source = x_ref.at[pl.ds(place, sub)]
        return pltpu.make_async_remote_copy(source, xs.at[pl.ds(pl.multiple_of(at, sub), sub)], ag_send.at[way, kind, s], ag_recv.at[way, kind, s],
                                            device_id={"tp": sides[way][0]}, device_id_type=MESH)

    def scatter(way, kind, buffer, turn_no, j):
        return pltpu.make_async_remote_copy(sends.at[way, buffer, j], recvs.at[way, kind, j], rs_send.at[way, turn_no, j],
                                            rs_recv.at[way, kind, j], device_id={"tp": sides[way][0]}, device_id_type=MESH)

    def project(index, places):
        for p, place in enumerate(places):
            @pl.loop(0, half // 16)
            def _(i):
                here = pl.ds(pl.multiple_of(place + i * 16, 16), 16)
                there = pl.ds(pl.multiple_of(p * half + i * 16, 16), 16)
                squares = jnp.zeros((16, span), jnp.float32)
                for c in range(spans):
                    wide = xs[here, c * span : (c + 1) * span].astype(jnp.float32)
                    squares += wide * wide
                scale = lax.rsqrt(jnp.sum(squares, -1, keepdims=True) * (1 / width) + 1e-6)
                for c in range(spans):
                    wide = xs[here, c * span : (c + 1) * span].astype(jnp.float32)
                    nb[there, c * span : (c + 1) * span] = (wide * scale * gain[:, c * span : (c + 1) * span]).astype(jnp.bfloat16)

        def body(j, slot):
            t = _dot(nb[:, :depth], wbuf[slot, 0])
            for c in range(1, PIECES):
                t += _dot(nb[:, c * depth : (c + 1) * depth], wbuf[slot, c])
            t = t.astype(jnp.bfloat16)
            for p, place in enumerate(places):
                here = pl.ds(place, half)
                for h in range(TILE // HEAD):
                    head = t[p * half : (p + 1) * half, h * HEAD : (h + 1) * HEAD]

                    @pl.when(j <= q_tiles)
                    def _():
                        wide = head.astype(jnp.float32)
                        turned = wide * turn[0, here, :] + pltpu.roll(wide, HEAD // 2, 1) * turn[1, here, :]
                        qkv[j * (TILE // HEAD) + h, here, :] = turned.astype(jnp.bfloat16)

                    @pl.when(j > q_tiles)
                    def _():
                        qkv[j * (TILE // HEAD) + h, here, :] = head

        stream(index, body)

    strips = [(g, list(range(g * group + i, min(g * group + i + 2, (g + 1) * group)))) for g in range(kv) for i in range(0, group, 2)]

    def attend(places):
        e = HEAD**-0.5 * LOG2E
        ones = jnp.ones((8, KEYS), jnp.bfloat16)

        @pl.loop(0, len(places))
        def _(unit):
            place = pl.multiple_of(jnp.where(unit == 0, places[0], places[1]), half)
            mine = pl.ds(place, half)
            top_s[...] = jnp.full(top_s.shape, HIDDEN, jnp.float32)
            mix_s[...] = jnp.zeros(mix_s.shape, jnp.float32)

            def block(j, masked):
                here = pl.ds(pl.multiple_of(j * KEYS, KEYS), KEYS)
                scores, weights, keeps = [], [], []
                for g, hs in strips:
                    q = jnp.concatenate([qkv[h, mine, :] for h in hs], axis=0)
                    scores.append(_dot(qkv[heads + g, here, :], q, 1, 1))
                if masked:
                    shape = (KEYS, 2 * half)
                    gap = lax.rem(lax.broadcasted_iota(jnp.int32, shape, 1), half) - lax.broadcasted_iota(jnp.int32, shape, 0)
                    ok = gap >= j * KEYS - place
                for i, s in enumerate(scores):
                    wide = s.shape[1]
                    if masked:
                        s = jnp.where(ok[:, :wide], s, HIDDEN)
                    old = top_s[i : i + 1, :wide]
                    top = jnp.maximum(old, s.max(axis=0, keepdims=True))
                    top_s[i : i + 1, :wide] = top
                    weights.append(jnp.exp2((s - top) * e).astype(jnp.bfloat16))
                    keeps.append(jnp.exp2((old - top) * e))
                for i, (g, hs) in enumerate(strips):
                    wide = len(hs) * half
                    values = jnp.concatenate([qkv[heads + kv + g, here, :].T, ones], axis=0)
                    mix_s[i, :, :wide] = mix_s[i, :, :wide] * keeps[i] + _dot(values, weights[i])

            whole = lax.div(place, KEYS)

            @pl.loop(0, whole)
            def _(j):
                block(j, False)

            block(whole, True)
            for i, (g, hs) in enumerate(strips):
                wide = len(hs) * half
                out = (mix_s[i, :HEAD, :wide] * (1 / mix_s[i, HEAD : HEAD + 1, :wide])).T.astype(jnp.bfloat16)
                for m, h in enumerate(hs):
                    qkv[h, mine, :] = out[m * half : (m + 1) * half, :]

    def terms(index, places, before, emit, during=None):
        for p, place in enumerate(places):
            for h in range(heads):
                nb[p * half : (p + 1) * half, h * HEAD : (h + 1) * HEAD] = qkv[h, pl.ds(place, half), :]

        def body(j, slot):
            before(j)
            for c in range(PIECES):
                emit(j, slice(c * TILE, (c + 1) * TILE), _dot(nb[:, :inner], wbuf[slot, c]))
                if during is not None and c == 0:
                    during(j)

        stream(index, body)

    def send_terms(index, places, kinds, turn_no):
        buffer = turn_no % 2

        def during(j):
            @pl.when(j > 0)
            def _():
                for way in range(2):
                    scatter(way, kinds[way], buffer, turn_no, j - 1).start()

        def before(j):
            if turn_no == 2:
                for way in range(2):
                    scatter(way, OWN, buffer, 0, j).wait_send()
                    scatter(way, VIA, buffer, turn_no, j).wait_recv()

        def emit(j, columns, t):
            for way in range(2):
                mine = t[way * half : (way + 1) * half]
                if turn_no == 2:
                    mine += recvs[way, VIA, j, :, columns].astype(jnp.float32)
                sends[way, buffer, j, :, columns] = mine.astype(jnp.bfloat16)

        terms(index, places, before, emit, during)
        for way in range(2):
            scatter(way, kinds[way], buffer, turn_no, spans - 1).start()

    barrier = pltpu.get_barrier_semaphore()
    pl.semaphore_signal(barrier, inc=1, device_id={"tp": left}, device_id_type=MESH)
    pl.semaphore_wait(barrier, 1)
    pass_first = (me > 0, me == n - 1)
    for way in range(2):
        if way == 1:
            pl.semaphore_signal(here_sem, inc=1, device_id={"tp": right}, device_id_type=MESH)
            pl.semaphore_wait(here_sem, 1)
        for s in range(2):
            gather(way, FIRST, s).start()
    load_x.start()
    load_gain.start()
    for j in range(SLOTS):
        passes[0](jnp.int32(j), j)
    load_turn.start()
    for s in range(2):
        for way in range(2):
            @pl.when(jnp.logical_not(pass_first[way]))
            def _():
                gather(way, SECOND, s).start()

    qkv[heads:] = jnp.zeros((2 * kv, *qkv.shape[1:]), jnp.bfloat16)
    load_x.wait()
    load_gain.wait()
    load_turn.wait()
    wide_gain = gain_in[...].astype(jnp.float32)
    for i in range(width // HEAD):
        gain[:, i * HEAD : (i + 1) * HEAD] = wide_gain[i : i + 1, :]
    project(0, (pl.multiple_of(me * rows, rows), pl.multiple_of(me * rows + half, half)))
    for s in range(2):
        for way in range(2):
            arrival(way, FIRST, s).wait_recv()
            gather(way, PASSED, s).start()
    for s in range(2):
        for way in range(2):
            @pl.when(pass_first[way])
            def _():
                gather(way, SECOND, s).start()
    project(1, (gathered(0, FIRST), gathered(1, FIRST)))

    second = (jnp.where(left > 0, PASSED, SECOND), jnp.where(right == n - 1, PASSED, SECOND))
    third = tuple(PASSED + SECOND - kind for kind in second)
    for index, kinds in ((2, second), (4, third)):
        for s in range(2):
            for way in range(2):
                arrival(way, kinds[way], s).wait_recv()
        project(index, (gathered(0, kinds[0]), gathered(1, kinds[1])))

        def scattered(way, kind):
            to = sides[way][0]
            return pl.multiple_of(jnp.where(kind == VIA, far * rows + (1 - way) * half,
                                            jnp.where(kind == OWN, to * rows + way * half, to * rows + (1 - way) * half)), half)

        early = tuple(jnp.where(sides[way][0] < far, OWN, VIA) for way in range(2))
        late = tuple(OWN + VIA - kind for kind in early)
        kinds = early if index == 2 else late
        places = tuple(scattered(way, kinds[way]) for way in range(2))
        attend(places)
        send_terms(index + 1, places, kinds, 0 if index == 2 else 1)

    kinds = (SUM, SUM)
    places = tuple(scattered(way, SUM) for way in range(2))
    attend(places)
    send_terms(6, places, kinds, 2)

    places = (pl.multiple_of(me * rows, rows), pl.multiple_of(me * rows + half, half))
    attend(places)

    def finish(j, columns, t):
        own[:, columns] = t
        if columns.stop < span:
            return
        at = pl.ds(pl.multiple_of(j * span, span), span)
        halves = (slice(0, half), slice(half, rows))
        for p in range(2):
            scatter(p, OWN, 0, 2, j).wait_recv()
            x_part = xs[pl.ds(pl.multiple_of(places[p], half), half), at].astype(jnp.float32)
            own[halves[p], :] = own[halves[p], :] + x_part + recvs[p, OWN, j].astype(jnp.float32)

        @pl.when(j > 0)
        def _():
            for way in range(2):
                scatter(way, SUM, 0, 2, j - 1).wait_send()

        for p in (0, 1):
            scatter(1 - p, SUM, 0, 2, j).wait_recv()
            y_ref[halves[p], at] = (own[halves[p], :] + recvs[1 - p, SUM, j].astype(jnp.float32)).astype(jnp.bfloat16)

    for way in range(2):
        for kind in (FIRST, PASSED, SECOND):
            for s in range(2):
                gather(way, kind, s).wait_send()

    @pl.loop(0, spans)
    def _(j):
        for way in range(2):
            scatter(way, late[way], 1, 1, j).wait_send()

    terms(7, places, lambda j: None, finish)
    for way in range(2):
        scatter(way, SUM, 0, 2, spans - 1).wait_send()


def _turns(tokens):
    half = HEAD // 2
    angle = np.arange(tokens, dtype=np.float32)[:, None] * np.float32(THETA) ** (-np.arange(half, dtype=np.float32) / np.float32(half))
    cos, sin = np.cos(angle.astype(np.float64)), np.sin(angle.astype(np.float64))
    return np.stack([np.concatenate([cos, cos], -1), np.concatenate([-sin, sin], -1)]).astype(np.float32)


def solution(mesh):
    n = mesh.shape["tp"]

    def step(x, gain, wq, wk, wv, wo):
        rows, width = x.shape
        inner, kv_inner = wq.shape[1], wk.shape[1]
        heads, kv = inner // HEAD, kv_inner // HEAD
        half, tokens, span = rows // 2, n * rows, PIECES * TILE
        spans, depth = width // span, width // PIECES
        strips = kv * -(-(heads // kv) // 2)
        bf16, f32 = jnp.bfloat16, jnp.float32
        anywhere = pl.BlockSpec(memory_space=pl.ANY)
        return pl.pallas_call(
            functools.partial(_kernel, n, heads, kv),
            out_shape=pltpu.VMEM((rows, width), bf16),
            in_specs=[anywhere] * 7,
            out_specs=pl.BlockSpec(memory_space=pltpu.VMEM),
            scratch_shapes=[
                pltpu.VMEM((tokens, width), bf16),
                pltpu.VMEM((rows, width), bf16),
                pltpu.VMEM((heads + 2 * kv, tokens, HEAD), bf16),
                pltpu.VMEM((2, 2, spans, half, span), bf16),
                pltpu.VMEM((2, 3, spans, half, span), bf16),
                pltpu.VMEM((rows, span), f32),
                pltpu.VMEM((SLOTS, PIECES, depth, TILE), bf16),
                pltpu.VMEM((2, tokens, HEAD), f32),
                pltpu.VMEM((width // HEAD, HEAD), bf16),
                pltpu.VMEM((1, width), f32),
                pltpu.VMEM((strips, 2 * half), f32),
                pltpu.VMEM((strips, HEAD + 8, 2 * half), f32),
                pltpu.SemaphoreType.DMA((2, 3, 2)),
                pltpu.SemaphoreType.DMA((2, 3, 2)),
                pltpu.SemaphoreType.DMA((2, 3, spans)),
                pltpu.SemaphoreType.DMA((2, 3, spans)),
                pltpu.SemaphoreType.DMA((SLOTS,)),
                pltpu.SemaphoreType.DMA((3,)),
                pltpu.SemaphoreType.REGULAR,
            ],
            compiler_params=pltpu.CompilerParams(collective_id=0, has_side_effects=True, vmem_limit_bytes=VMEM),
        )(x, gain.reshape(width // HEAD, HEAD), _turns(tokens), wq.reshape(PIECES, depth, inner), wk.reshape(PIECES, depth, kv_inner),
          wv.reshape(PIECES, depth, kv_inner), wo)

    tokens, columns = P(("dp", "tp"), None), P(None, "tp")
    return jax.shard_map(
        step,
        mesh=mesh,
        in_specs=(tokens, P(None), columns, columns, columns, P("tp", None)),
        out_specs=tokens,
        check_vma=False,
    )
```
